128 devices in a mesh: space: 16 (over z_lo, y, core), mode: 8 (over x, z_hi).
Axes of the slice: x: 4, y: 4, z: 4 (z_hi: 2, z_lo: 2; z = z_hi * 2 + z_lo), core: 2. Of those that a mesh axis runs over, the one named last changes fastest.
Arguments:
- test_modes: float32 [32, 3, 8, 32, 256], P(None, None, None, 'space'), may hold values from -6 to 6
- modes: float32 [128, 3, 8, 32, 256], P('mode', None, None, 'space'), may hold values from -6 to 6
Outputs:
- triad: float32 [32, 128, 128], P('space', 'mode')
The draws below stay inside these ranges and needn't reach their ends.
All inputs are finite; a program needn't handle non-finite values.
Results may differ from the reference program's by a relative error of at most 0.000071.
Values sent between devices are 32-bit elements; how exact they have to be, the bound alone decides.
A program may use at most 64 MiB of HBM per device.

```python
import math
import jax
import jax.numpy as jnp
from jax import lax

MODES = 128
I_BLK = 32
NX = 256
NZ = 8
NY = 32


def levels(own_key, shape, split, least, high):
    loudness, own = 1.0, jax.random.fold_in(own_key, 6)
    for position, blocks in split:
        steps = jnp.exp(jax.random.uniform(jax.random.fold_in(own, position), (blocks,), jnp.float32, least / len(split), high / len(split)))
        loudness = loudness * jnp.repeat(steps, shape[position] // blocks).reshape([-1 if axis == position else 1 for axis in range(len(shape))])
    return loudness


def bell_draw(own_key, dims, scale, bound, cuts=(), kind=jnp.bfloat16):
    drawn = scale * jax.random.normal(own_key, dims, jnp.float32)
    if cuts:
        drawn = drawn * levels(own_key, dims, cuts, -0.22, 0.18)
    return jnp.clip(drawn, -bound, bound).astype(kind)


def setup_inputs(seed: int = 0) -> dict:
    key_of = jax.random.split(jax.random.key(seed), 3)
    return {
        "test_modes": bell_draw(key_of[0], (I_BLK, 3, NZ, NY, NX), 1.0, 6.0, ((3, 16),), jnp.float32),
        "modes": bell_draw(key_of[1], (MODES, 3, NZ, NY, NX), 1.0, 6.0, ((0, 8), (3, 16)), jnp.float32),
    }


def central_diff(field, along):
    ahead = jnp.roll(field, -1, along) - jnp.roll(field, 1, along)
    farther = jnp.roll(field, -2, along) - jnp.roll(field, 2, along)
    return (8.0 * ahead - farther) / 12.0

def reference(test_modes, modes):
    volume_scale = 1.0 / math.sqrt(NX * NY * NZ)
    test_flat = test_modes.reshape(I_BLK, 3, -1)
    mode_flat = modes.reshape(MODES, 3, -1)

    def one_mode(field):
        gradients = jnp.stack([central_diff(field, 3), central_diff(field, 2), central_diff(field, 1)], axis=1)
        gradients = gradients.reshape(3, 3, -1)
        weighted = test_flat[:, 0, None, :] * gradients[0][None]
        weighted = weighted + test_flat[:, 1, None, :] * gradients[1][None]
        weighted = weighted + test_flat[:, 2, None, :] * gradients[2][None]
        return jnp.einsum('ibc,jbc->ij', weighted, mode_flat, precision=lax.Precision.HIGHEST)
    stacked = lax.map(one_mode, modes)
    return jnp.transpose(stacked, (1, 0, 2)) * volume_scale
```

```python
import functools

import jax
import jax.numpy as jnp
from jax import lax
from jax.experimental import pallas as pl
from jax.experimental.pallas import tpu as pltpu
from jax.sharding import PartitionSpec as P

F32 = jnp.float32
BF16 = jnp.bfloat16
MESH = pl.DeviceIdType.MESH
SCALE = 1.0 / 12.0 / 256.0
TILES = 14
ORDERS = ((0, 1, 2), (1, 2, 0), (2, 0, 1), (0, 2, 1))


def kernel(test_hbm, mode_hbm, out_ref, x_modes, x_tests, sent, got, up, down, tests, grads,
           rhs, part, paired, land1, sum1, land2, sum2, land3, load_sem, a2a_send, a2a_recv,
           up_send, down_send, up_recv, down_recv, pair_send, pair_recv, red_send, red_recv):
    s = lax.axis_index("space")
    m = lax.axis_index("mode")
    core = s % 2
    cy = (s // 2) % 4
    zlo = s // 8
    cx = m // 2
    cz = (m % 2) * 2 + zlo
    place = (cx, cy, cz)

    def device(x, y, z, c):
        return ((z % 2) * 8 + y * 2 + c, x * 2 + z // 2)

    def shifted(axis, step):
        there = list(place)
        there[axis] = (there[axis] + step) % 4
        return device(*there, core)

    load_modes = pltpu.make_async_copy(mode_hbm, x_modes, load_sem.at[0])
    load_tests = pltpu.make_async_copy(test_hbm, x_tests, load_sem.at[1])
    load_modes.start()
    load_tests.start()

    barrier = pltpu.get_barrier_semaphore()
    above = (s + 1) % 16
    below = (s + 15) % 16
    friends = [(s, (m + p) % 8) for p in range(1, 8)]
    friends += [(above, m), (below, m)]
    friends += [shifted(1, p) for p in range(1, 4)]
    friends += [shifted(2, p) for p in (1, 3)]
    for friend in friends:
        pl.semaphore_signal(barrier, inc=1, device_id=friend, device_id_type=MESH)

    lane = lax.broadcasted_iota(jnp.int32, (8, 128), 1)
    within = lane % 32
    low_half = lane < 64
    even_group = (lane // 32) % 2 == 0

    load_modes.wait()

    def arrange(at, carry):
        row = (at // 4) * 32 + (at % 4) * 4
        for xt in range(2):
            for kh in range(2):
                rows = [
                    x_modes[pl.ds(row + kh * 768 + (g // 2) * 16 + xt * 2 + g % 2, 8, stride=96), :]
                    for g in range(4)
                ]
                halves = []
                for g in range(2):
                    halves.append(jnp.where(low_half, rows[g], pltpu.roll(rows[g + 2], 64, 1)))
                for g in range(2):
                    halves.append(jnp.where(low_half, pltpu.roll(rows[g], 64, 1), rows[g + 2]))
                for c in range(2):
                    b0, b1 = halves[2 * c], halves[2 * c + 1]
                    first = jnp.where(even_group, b0, pltpu.roll(b1, 32, 1))
                    second = jnp.where(even_group, pltpu.roll(b0, 96, 1), b1)
                    sent[xt * 4 + 2 * c, at, pl.ds(kh * 8, 8), :] = first
                    sent[xt * 4 + 2 * c + 1, at, pl.ds(kh * 8, 8), :] = second
        return carry

    lax.fori_loop(0, 12, arrange, 0)

    def edges(d, carry):
        left, right = (d + 7) % 8, (d + 1) % 8
        for kh in range(2):
            rows = pl.ds(kh * 8, 8)
            for pack in range(2):
                packed = jnp.zeros((8, 128), F32)
                for slot in range(8 if pack == 0 else 4):
                    at = pack * 8 + slot
                    turn = 4 * slot - 30
                    from_left = pltpu.roll(sent[left, at, rows, :], (turn - 32) % 128, 1)
                    from_right = pltpu.roll(sent[right, at, rows, :], (turn + 32) % 128, 1)
                    spot = within - 4 * slot
                    packed = jnp.where((spot == 0) | (spot == 1), from_left, packed)
                    packed = jnp.where((spot == 2) | (spot == 3), from_right, packed)
                sent[d, 12 + pack, rows, :] = packed
        return carry

    lax.fori_loop(0, 8, edges, 0)

    pl.semaphore_wait(barrier, len(friends))

    def to_peer(p):
        return pltpu.make_async_remote_copy(
            src_ref=sent.at[(m + p) % 8], dst_ref=got.at[m],
            send_sem=a2a_send.at[p - 1], recv_sem=a2a_recv.at[p - 1],
            device_id=(s, (m + p) % 8), device_id_type=MESH)

    def to_above(p, src):
        k = (m + 8 - p) % 8
        return pltpu.make_async_remote_copy(
            src_ref=src, dst_ref=down.at[k], send_sem=up_send.at[p], recv_sem=down_recv.at[p],
            device_id=(above, m), device_id_type=MESH)

    def to_below(p, src):
        k = (m + 8 - p) % 8
        return pltpu.make_async_remote_copy(
            src_ref=src, dst_ref=up.at[k], send_sem=down_send.at[p], recv_sem=up_recv.at[p],
            device_id=(below, m), device_id_type=MESH)

    def start_peer(p, carry):
        to_peer(p).start()
        return carry

    lax.fori_loop(1, 8, start_peer, 0)
    own = sent.at[m, pl.ds(0, 12)]
    to_above(0, own).start()
    to_below(0, own).start()

    load_tests.wait()
    xt_mine, c_mine = m // 4, m % 4

    def arrange_tests(at, carry):
        row = (at // 4) * 32 + (at % 4) * 4 + xt_mine * 2
        for ih in range(4):
            value = None
            for g in range(4):
                line = x_tests[pl.ds(row + ih * 768 + (g // 2) * 16 + g % 2, 8, stride=96), :]
                line = pltpu.roll(line, (32 * g - 32 * c_mine + 128) % 128, 1)
                value = line if value is None else jnp.where(lane // 32 == g, line, value)
            tests[at, pl.ds(ih * 8, 8), :] = value
        return carry

    lax.fori_loop(0, 12, arrange_tests, 0)

    def split(value):
        high = value.astype(BF16)
        return high, (value - high.astype(F32)).astype(BF16)

    lane16 = lax.broadcasted_iota(jnp.int32, (16, 128), 1)
    in16 = lane16 % 32

    def first_grads(k):
        rows = pl.ds(pl.multiple_of(k * 16, 16), 16)
        for a in range(3):
            packed = got[k, 12 + a // 2]
            field = [got[k, a * 4 + t] for t in range(4)]
            turned = [pltpu.roll(f, 64, 1) for f in field]
            for t in range(4):
                f = field[t]
                slot = (a % 2) * 4 + t
                turn = 30 - 4 * slot

                def at_edge(step, edge):
                    moved = pltpu.roll(f, step % 128, 1)
                    halo = pltpu.roll(packed, (turn + step) % 128, 1)
                    return jnp.where(edge, halo, moved)

                near = at_edge(-1, in16 == 31) - at_edge(1, in16 == 0)
                far = at_edge(-2, in16 >= 30) - at_edge(2, in16 <= 1)
                grads[0, a, t, rows, :] = (8.0 * near - far) * SCALE

                def along_z(step):
                    n = t + step
                    return field[n] if 0 <= n < 4 else turned[n % 4]

                near = along_z(1) - along_z(-1)
                far = along_z(2) - along_z(-2)
                grads[2, a, t, rows, :] = (8.0 * near - far) * SCALE

    even16 = (lane16 // 32) % 2 == 0

    def second_grads(k):
        rows = pl.ds(pl.multiple_of(k * 16, 16), 16)
        for a in range(3):
            for t in range(4):
                here, over, under = got[k, a * 4 + t], up[k, a * 4 + t], down[k, a * 4 + t]
                before = pltpu.roll(here - under, 96, 1)
                after = pltpu.roll(over - here, 32, 1)
                near = jnp.where(even16, before, after)
                grads[1, a, t, rows, :] = (8.0 * near + (under - over)) * SCALE

    got[m] = sent[m]
    first_grads(m)

    def arrival(p, carry):
        k = (m + 8 - p) % 8
        to_peer(p).wait_recv()
        block = got.at[k, pl.ds(0, 12)]
        to_above(p, block).start()
        to_below(p, block).start()
        first_grads(k)
        return carry

    lax.fori_loop(1, 8, arrival, 0)

    def turn_modes(at, carry):
        field = got[:, at].reshape(128, 128).T
        high, low = split(field)
        rows = pl.ds(pl.multiple_of(at * 128, 128), 128)
        rhs[rows, 0:128] = high
        rhs[rows, 128:256] = low
        return carry

    lax.fori_loop(0, 12, turn_modes, 0)

    def triad_of(n, components):
        c = jnp.where(n < 8, 1 - core, core)
        y, zl = (n // 2) % 4, n % 2
        pair = zl * 8 + y * 2 + c
        total = None
        for b in components:
            for tp in range(2):
                columns = []
                for t in (2 * tp, 2 * tp + 1):
                    blocks = []
                    for r in range(2):
                        value = None
                        for a in range(3):
                            line = tests[a * 4 + t, pl.ds(pair * 2 + r, 1), :]
                            term = line * grads[b, a, t]
                            value = term if value is None else value + term
                        blocks.append(value)
                    columns.append(jnp.concatenate(blocks, axis=0))
                high, low = split(jnp.concatenate(columns, axis=1))
                left = jnp.concatenate([high, low], axis=0)
                right = rhs[(b * 4 + 2 * tp) * 128 : (b * 4 + 2 * tp + 2) * 128, :]
                piece = jnp.dot(left, right, preferred_element_type=F32)
                total = piece if total is None else total + piece
        value = (total[:256, :128] + total[:256, 128:]) + (total[256:, :128] + total[256:, 128:])
        return c, y, zl, value

    def spots(c, y, zl, x, zh, q):
        where = (x, y, zh * 2 + zl)
        first, second, third = ORDERS[q]
        return q, c, where[first], where[second], where[third]

    def phase1(n, carry):
        c, y, zl, value = triad_of(n, (0, 2))
        for r in range(2):
            for v in range(16):
                spot = spots(c, y, zl, v // 4, (v // 2) % 2, r * 2 + v % 2)
                part[spot] = value[r * 128 + v * 8 : r * 128 + v * 8 + 8]
        return carry

    def phase2(n, carry):
        c, y, zl, value = triad_of(n, (1,))
        for r in range(2):
            for v in range(16):
                spot = spots(c, y, zl, v // 4, (v // 2) % 2, r * 2 + v % 2)
                part[spot] = part[spot] + value[r * 128 + v * 8 : r * 128 + v * 8 + 8]
        return carry

    lax.fori_loop(0, 16, phase1, 0)

    def halo(p, carry):
        k = (m + 8 - p) % 8
        block = got.at[k, pl.ds(0, 12)]
        to_above(p, block).wait_recv()
        to_below(p, block).wait_recv()
        second_grads(k)
        return carry

    lax.fori_loop(0, 8, halo, 0)

    def to_pair(q):
        return pltpu.make_async_remote_copy(
            src_ref=part.at[q, 1 - core], dst_ref=paired.at[q],
            send_sem=pair_send.at[q], recv_sem=pair_recv.at[q],
            device_id=device(cx, cy, cz, 1 - core), device_id_type=MESH)

    lax.fori_loop(0, 8, phase2, 0)
    for q in range(4):
        to_pair(q).start()
    lax.fori_loop(8, 16, phase2, 0)

    sources = (None, sum1, sum2)
    landings = (land1, land2, land3)

    def to_owner(q, stage, p):
        axis = ORDERS[q][stage]
        there = (place[axis] + p) % 4
        src = part.at[q, core, there] if stage == 0 else sources[stage].at[q, there]
        return pltpu.make_async_remote_copy(
            src_ref=src, dst_ref=landings[stage].at[q, p - 1],
            send_sem=red_send.at[stage, q, p - 1], recv_sem=red_recv.at[stage, q, p - 1],
            device_id=shifted(axis, p), device_id_type=MESH)

    for q in range(4):
        to_pair(q).wait_recv()
        part[q, core] = part[q, core] + paired[q]
        for p in range(1, 4):
            to_owner(q, 0, p).start()
    for stage in range(3):
        for q in range(4):
            for p in range(1, 4):
                to_owner(q, stage, p).wait_recv()
            mine = place[ORDERS[q][stage]]
            kept = part[q, core, mine] if stage == 0 else sources[stage][q, mine]
            landing = landings[stage]
            value = (kept + landing[q, 0]) + (landing[q, 1] + landing[q, 2])
            if stage == 2:
                out_ref[q // 2, pl.ds((q % 2) * 8, 8), :] = value
            else:
                sources[stage + 1][q] = value
                for p in range(1, 4):
                    to_owner(q, stage + 1, p).start()

    def end_peer(p, carry):
        to_peer(p).wait_send()
        return carry

    def end_halo(p, carry):
        to_above(p, own).wait_send()
        to_below(p, own).wait_send()
        return carry

    lax.fori_loop(1, 8, end_peer, 0)
    lax.fori_loop(0, 8, end_halo, 0)
    for q in range(4):
        to_pair(q).wait_send()
        for stage in range(3):
            for p in range(1, 4):
                to_owner(q, stage, p).wait_send()


def per_device(test_modes, modes):
    def lines(value):
        count = value.shape[0]
        value = value.reshape(count, 3, 8, 2, 2, 128).transpose(0, 1, 2, 4, 3, 5)
        return value.reshape(count * 96, 128)

    dma = pltpu.SemaphoreType.DMA
    return pl.pallas_call(
        kernel,
        out_shape=jax.ShapeDtypeStruct((2, 16, 128), F32),
        in_specs=[pl.BlockSpec(memory_space=pl.ANY)] * 2,
        out_specs=pl.BlockSpec(memory_space=pltpu.VMEM),
        scratch_shapes=[
            pltpu.VMEM((1536, 128), F32),
            pltpu.VMEM((3072, 128), F32),
            pltpu.VMEM((8, TILES, 16, 128), F32),
            pltpu.VMEM((8, TILES, 16, 128), F32),
            pltpu.VMEM((8, 12, 16, 128), F32),
            pltpu.VMEM((8, 12, 16, 128), F32),
            pltpu.VMEM((12, 32, 128), F32),
            pltpu.VMEM((3, 3, 4, 128, 128), F32),
            pltpu.VMEM((1536, 256), BF16),
            pltpu.VMEM((4, 2, 4, 4, 4, 8, 128), F32),
            pltpu.VMEM((4, 4, 4, 4, 8, 128), F32),
            pltpu.VMEM((4, 3, 4, 4, 8, 128), F32),
            pltpu.VMEM((4, 4, 4, 8, 128), F32),
            pltpu.VMEM((4, 3, 4, 8, 128), F32),
            pltpu.VMEM((4, 4, 8, 128), F32),
            pltpu.VMEM((4, 3, 8, 128), F32),
            dma((2,)),
            dma((7,)),
            dma((7,)),
            dma((8,)),
            dma((8,)),
            dma((8,)),
            dma((8,)),
            dma((4,)),
            dma((4,)),
            dma((3, 4, 3)),
            dma((3, 4, 3)),
        ],
        compiler_params=pltpu.CompilerParams(
            collective_id=0, has_side_effects=True, vmem_limit_bytes=48 * 1024 * 1024),
    )(lines(test_modes), lines(modes))


def solution(mesh):
    in_specs = (P(None, None, None, "space", None), P("mode", None, None, "space", None))
    out_specs = P("space", "mode", None)
    return jax.shard_map(
        per_device, mesh=mesh, in_specs=in_specs, out_specs=out_specs, check_vma=False
    )
```

```python
import jax
import jax.numpy as jnp
from jax import lax
from jax.experimental import pallas as pl
from jax.experimental.pallas import tpu as pltpu
from jax.sharding import PartitionSpec as P

F32 = jnp.float32
BF16 = jnp.bfloat16
MESH = pl.DeviceIdType.MESH
SCALE = 1.0 / 12.0 / 256.0
X, Y, Z = 0, 1, 2
ORDERS = ((X, Y, Z), (Y, Z, X), (Z, X, Y), (Y, X, Z))


def rem(value, size):
    return lax.rem(value, jnp.int32(size)) if isinstance(value, jax.Array) else value % size


def div(value, size):
    return lax.div(value, jnp.int32(size)) if isinstance(value, jax.Array) else value // size


def kernel(test_hbm, mode_hbm, out_ref, x_modes, x_tests, sent, got, up, down, tests, lent,
           grads, rhs, part, paired, land1, sum1, land2, sum2, land3, load_sem, a2a_send, a2a_recv,
           up_send, down_send, up_recv, down_recv, test_send, test_recv, pair_send, pair_recv, red_send, red_recv):
    s = lax.axis_index("space")
    m = lax.axis_index("mode")
    core = rem(s, 2)
    cy = rem(div(s, 2), 4)
    zlo = div(s, 8)
    cx = div(m, 2)
    zhi = rem(m, 2)
    cz = zhi * 2 + zlo
    place = (cx, cy, cz)

    def device(x, y, z, c):
        return (rem(z, 2) * 8 + y * 2 + c, x * 2 + div(z, 2))

    def shifted(axis, step):
        there = list(place)
        there[axis] = rem(there[axis] + step, 4)
        return device(*there, core)

    load_modes = pltpu.make_async_copy(mode_hbm, x_modes, load_sem.at[0])
    load_tests = pltpu.make_async_copy(test_hbm, x_tests, load_sem.at[1])
    load_modes.start()
    load_tests.start()

    barrier = pltpu.get_barrier_semaphore()
    spot = cy * 2 + core

    def ring(step):
        there = rem(spot + step + 8, 8)
        return device(cx, div(there, 2), cz, rem(there, 2))

    def in_plane(n):
        return device(rem(cx + div(n, 4), 4), cy, rem(cz + rem(n, 4), 4), core)

    friends = [in_plane(n) for n in range(1, 16)]
    friends += [ring(1), ring(-1)]
    friends += [shifted(Y, p) for p in range(1, 4)]
    for friend in friends:
        pl.semaphore_signal(barrier, inc=1, device_id=friend, device_id_type=MESH)

    lane = lax.broadcasted_iota(jnp.int32, (8, 128), 1)
    within = lane % 16
    group = lane // 16

    load_modes.wait()

    def arrange(n, carry):
        y, a = div(n, 3), rem(n, 3)
        for xt in range(2):
            for kh in range(2):
                rows = [
                    x_modes[pl.ds(a * 32 + y + kh * 768 + z * 4 + xt * 2, 8, stride=96), :]
                    for z in range(8)
                ]
                for step in (4, 2, 1):
                    low = (group // step) % 2 == 0
                    for z in range(8):
                        if (z // step) % 2 == 0:
                            first, second = rows[z], rows[z + step]
                            rows[z] = jnp.where(low, first, pltpu.roll(second, 16 * step, 1))
                            rows[z + step] = jnp.where(
                                low, pltpu.roll(first, 128 - 16 * step, 1), second)
                for c in range(8):
                    sent[xt * 8 + c, n, pl.ds(kh * 8, 8), :] = rows[c]
        return carry

    lax.fori_loop(0, 6, arrange, 0)

    def edges(d, carry):
        left, right = rem(d + 15, 16), rem(d + 1, 16)
        for y in range(2):
            for kh in range(2):
                rows = pl.ds(kh * 8, 8)
                packed = jnp.zeros((8, 128), F32)
                for slot in range(3):
                    turn = 4 * slot - 14
                    from_left = pltpu.roll(sent[left, y * 3 + slot, rows, :], (turn - 16) % 128, 1)
                    from_right = pltpu.roll(sent[right, y * 3 + slot, rows, :], (turn + 16) % 128, 1)
                    place_in = within - 4 * slot
                    packed = jnp.where((place_in == 0) | (place_in == 1), from_left, packed)
                    packed = jnp.where((place_in == 2) | (place_in == 3), from_right, packed)
                sent[d, 6 + y, rows, :] = packed
        return carry

    lax.fori_loop(0, 16, edges, 0)

    pl.semaphore_wait(barrier, len(friends))

    def source(n):
        x, z = rem(cx + 4 - div(n, 4), 4), rem(cz + 4 - rem(n, 4), 4)
        return rem(z, 2), x * 2 + div(z, 2)

    def to_peer(n):
        column = rem(cx + div(n, 4), 4) * 4 + rem(cz + rem(n, 4), 4)
        return pltpu.make_async_remote_copy(
            src_ref=sent.at[column], dst_ref=got.at[zlo, m],
            send_sem=a2a_send.at[n], recv_sem=a2a_recv.at[n],
            device_id=in_plane(n), device_id_type=MESH)

    def to_above(n, src):
        slab, k = source(n)
        slab = rem(slab + div(spot, 7), 2)
        return pltpu.make_async_remote_copy(
            src_ref=src, dst_ref=down.at[slab, k],
            send_sem=up_send.at[n], recv_sem=down_recv.at[slab * 8 + k],
            device_id=ring(1), device_id_type=MESH)

    def to_below(n, src):
        slab, k = source(n)
        slab = rem(slab + div(7 - spot, 7), 2)
        return pltpu.make_async_remote_copy(
            src_ref=src, dst_ref=up.at[slab, k],
            send_sem=down_send.at[n], recv_sem=up_recv.at[slab * 8 + k],
            device_id=ring(-1), device_id_type=MESH)

    def from_ring(slab, k):
        for buffer, sems, sends in ((down, down_recv, up_send), (up, up_recv, down_send)):
            pltpu.make_async_remote_copy(
                src_ref=got.at[slab, k, pl.ds(0, 6)], dst_ref=buffer.at[slab, k],
                send_sem=sends.at[0], recv_sem=sems.at[slab * 8 + k],
                device_id=ring(1), device_id_type=MESH).wait_recv()

    own = sent.at[cx * 4 + cz, pl.ds(0, 6)]
    for n in range(1, 16):
        to_peer(n).start()
    to_above(0, own).start()
    to_below(0, own).start()

    load_tests.wait()

    def arrange_tests(y):
        c_mine = rem(cx, 2) * 4 + cz
        c_lent = rem(cx, 2) * 4 + rem(cz + (1 if y == 0 else 3), 4)

        def one(a, carry):
            for ih in range(4):
                start = a * 32 + y + div(cx, 2) * 2 + ih * 768
                turned = [
                    pltpu.roll(x_tests[pl.ds(start + z * 4, 8, stride=96), :], 16 * z, 1)
                    if z else x_tests[pl.ds(start, 8, stride=96), :]
                    for z in range(8)
                ]

                def pick(c):
                    value = turned[0]
                    for z in range(1, 8):
                        value = jnp.where((group + 8 - z) % 8 == c, turned[z], value)
                    return pltpu.roll(value, (128 - 16 * c) % 128, 1)

                rows = pl.ds(ih * 8, 8)
                tests[zlo, y, a, rows, :] = pick(c_mine)
                lent[y, a, rows, :] = pick(c_lent)
            return carry

        lax.fori_loop(0, 3, one, 0)

    def to_borrower(y):
        return pltpu.make_async_remote_copy(
            src_ref=lent.at[y], dst_ref=tests.at[zlo, y],
            send_sem=test_send.at[y], recv_sem=test_recv.at[y],
            device_id=shifted(Z, 1 if y == 0 else 3), device_id_type=MESH)

    def wait_tests(y):
        pltpu.make_async_remote_copy(
            src_ref=lent.at[y], dst_ref=tests.at[1 - zlo, y],
            send_sem=test_send.at[y], recv_sem=test_recv.at[y],
            device_id=shifted(Z, 1 if y == 0 else 3), device_id_type=MESH).wait_recv()

    for y in range(2):
        arrange_tests(y)
        to_borrower(y).start()

    def split(value):
        high = value.astype(BF16)
        return high, (value - high.astype(F32)).astype(BF16)

    in16 = lax.broadcasted_iota(jnp.int32, (16, 128), 1) % 16

    def first_grads(n, y):
        slab, k = source(n)
        rows = pl.ds(pl.multiple_of(k * 16, 16), 16)
        packed = got[slab, k, 6 + y]
        for a in range(3):
            f = got[slab, k, y * 3 + a]
            near = pltpu.roll(f, 112, 1) - pltpu.roll(f, 16, 1)
            far = pltpu.roll(f, 96, 1) - pltpu.roll(f, 32, 1)
            grads[2, y, a, slab, rows, :] = (8.0 * near - far) * SCALE

            def at_edge(step, edge):
                moved = pltpu.roll(f, step % 128, 1)
                halo = pltpu.roll(packed, (14 - 4 * a + step) % 128, 1)
                return jnp.where(edge, halo, moved)

            near = at_edge(-1, in16 == 15) - at_edge(1, in16 == 0)
            far = at_edge(-2, in16 >= 14) - at_edge(2, in16 <= 1)
            grads[0, y, a, slab, rows, :] = (8.0 * near - far) * SCALE

    def second_grads(n):
        slab, k = source(n)
        from_ring(slab, k)
        rows = pl.ds(pl.multiple_of(k * 16, 16), 16)
        for a in range(3):
            f0, f1 = got[slab, k, a], got[slab, k, 3 + a]
            f2, f3 = up[slab, k, a], up[slab, k, 3 + a]
            b2, b1 = down[slab, k, a], down[slab, k, 3 + a]
            grads[1, 0, a, slab, rows, :] = (8.0 * (f1 - b1) - (f2 - b2)) * SCALE
            grads[1, 1, a, slab, rows, :] = (8.0 * (f2 - f0) - (f3 - b1)) * SCALE

    def arrival(n):
        slab, k = source(n)
        to_peer(n).wait_recv()
        block = got.at[slab, k, pl.ds(0, 6)]
        to_above(n, block).start()
        to_below(n, block).start()

    def turn_modes(y):
        def turn_tile(n, carry):
            field = got[rem(n, 2), :, y * 3 + div(n, 2)].reshape(128, 128).T
            high, low = split(field)
            rows = pl.ds(pl.multiple_of((div(n, 2) * 4 + y * 2 + rem(n, 2)) * 128, 128), 128)
            rhs[rows, 0:128] = high
            rhs[rows, 128:256] = low
            return carry

        lax.fori_loop(0, 6, turn_tile, 0)

    def triads(c, y, terms):
        total = None
        for b, row in terms:
            columns = []
            for slab in range(2):
                blocks = []
                for zl in range(2):
                    for r in range(2):
                        i = (zl * 8 + y * 2 + c) * 2 + r
                        value = None
                        for a in range(3):
                            line = tests[slab, row, a, pl.ds(i, 1), :]
                            term = line * grads[b, row, a, slab]
                            value = term if value is None else value + term
                        blocks.append(value)
                columns.append(blocks)
            pieces = []
            for n in range(4):
                high, low = split(jnp.concatenate([columns[0][n], columns[1][n]], axis=1))
                pieces += [high, low]
            left = jnp.concatenate(pieces, axis=0)
            right = rhs[(b * 4 + row * 2) * 128 : (b * 4 + row * 2 + 2) * 128, :]
            piece = jnp.dot(left, right, preferred_element_type=F32)
            total = piece if total is None else total + piece
        values = []
        for n in range(4):
            high, low = total[n * 256 : n * 256 + 128], total[n * 256 + 128 : n * 256 + 256]
            values.append((high[:, :128] + high[:, 128:]) + (low[:, :128] + low[:, 128:]))
        return values

    def step(c, y, terms, add):
        values = triads(c, y, terms)
        for n in range(4):
            zl, r = n // 2, n % 2
            for v in range(16):
                spot = (r * 2 + v % 2, c, y, v // 4, zl * 2 + (v // 2) % 2)
                piece = values[n][v * 8 : v * 8 + 8]
                part[spot] = part[spot] + piece if add else piece

    got[zlo, m] = sent[cx * 4 + cz]
    first_grads(0, 0)
    first_grads(0, 1)

    def arrivals(n, carry):
        arrival(n)
        first_grads(n, 0)
        first_grads(n, 1)
        return carry

    lax.fori_loop(1, 16, arrivals, 0)
    for y in range(2):
        turn_modes(y)
        wait_tests(y)

    def phase1(p, carry):
        step(rem(p, 2), div(p, 2), ((0, 0), (2, 0), (0, 1), (2, 1)), False)
        return carry

    lax.fori_loop(0, 8, phase1, 0)

    def halos(n, carry):
        second_grads(n)
        return carry

    lax.fori_loop(0, 16, halos, 0)

    def plane(z):
        return rem(z, 2) * 2 + div(z, 2)

    def spot_of(axis, step):
        there = rem(place[axis] + step, 4)
        return plane(there) if axis == Z else there

    def to_pair(y):
        return pltpu.make_async_remote_copy(
            src_ref=part.at[:, 1 - core, y], dst_ref=paired.at[y],
            send_sem=pair_send.at[y], recv_sem=pair_recv.at[y],
            device_id=device(cx, cy, cz, 1 - core), device_id_type=MESH)

    def first_sum(q, p, y):
        axis = ORDERS[q][0]
        there = spot_of(axis, p)
        if axis == Y:
            src, dst = part.at[q, core, y], land1.at[q, p - 1]
        elif axis == X:
            src, dst = part.at[q, core, y, there], land1.at[q, p - 1, y]
        else:
            src, dst = part.at[q, core, y, :, there], land1.at[q, p - 1, y]
        return pltpu.make_async_remote_copy(
            src_ref=src, dst_ref=dst,
            send_sem=red_send.at[0, q, p - 1], recv_sem=red_recv.at[0, q, p - 1],
            device_id=shifted(axis, p), device_id_type=MESH)

    def first_wait(q, p):
        axis = ORDERS[q][0]
        return pltpu.make_async_remote_copy(
            src_ref=sum1.at[q], dst_ref=land1.at[q, p - 1],
            send_sem=red_send.at[0, q, p - 1], recv_sem=red_recv.at[0, q, p - 1],
            device_id=shifted(axis, p), device_id_type=MESH)

    def finish_group(g):
        y = rem(cy + g + 1, 4)
        to_pair(y).wait_recv()
        for q in range(4):
            part[q, core, y] = part[q, core, y] + paired[y, q]
        for q in range(4):
            if ORDERS[q][0] == Y:
                if g < 3:
                    first_sum(q, g + 1, y).start()
            else:
                for p in range(1, 4):
                    first_sum(q, p, y).start()

    for g in range(4):
        y = rem(cy + g + 1, 4)

        def phase3(h, carry):
            c = jnp.where(h == 0, 1 - core, core)
            step(c, y, ((1, 0), (1, 1)), True)

            @pl.when(h == 0)
            def _():
                to_pair(y).start()

            return carry

        lax.fori_loop(0, 2, phase3, 0)
        if g > 0:
            finish_group(g - 1)
    finish_group(3)

    def dims_after(q):
        return [axis for axis in (Y, X, Z) if axis != ORDERS[q][0]]

    def second_sum(q, p):
        axis = ORDERS[q][1]
        there = spot_of(axis, p)
        src = sum1.at[q, there] if dims_after(q)[0] == axis else sum1.at[q, :, there]
        return pltpu.make_async_remote_copy(
            src_ref=src, dst_ref=land2.at[q, p - 1],
            send_sem=red_send.at[1, q, p - 1], recv_sem=red_recv.at[1, q, p - 1],
            device_id=shifted(axis, p), device_id_type=MESH)

    def third_sum(q, p):
        axis = ORDERS[q][2]
        return pltpu.make_async_remote_copy(
            src_ref=sum2.at[q, spot_of(axis, p)], dst_ref=land3.at[q, p - 1],
            send_sem=red_send.at[2, q, p - 1], recv_sem=red_recv.at[2, q, p - 1],
            device_id=shifted(axis, p), device_id_type=MESH)

    def added(kept, landing):
        return (kept + landing[0]) + (landing[1] + landing[2])

    for q in range(4):
        for p in range(1, 4):
            first_wait(q, p).wait_recv()
        axis = ORDERS[q][0]
        mine = spot_of(axis, 0)
        if axis == Y:
            kept = part[q, core, mine]
        elif axis == X:
            kept = part[q, core, :, mine]
        else:
            kept = part[q, core, :, :, mine]
        sum1[q] = added(kept, [land1[q, n] for n in range(3)])
        for p in range(1, 4):
            second_sum(q, p).start()
    for q in range(4):
        for p in range(1, 4):
            second_sum(q, p).wait_recv()
        axis = ORDERS[q][1]
        mine = spot_of(axis, 0)
        kept = sum1[q, mine] if dims_after(q)[0] == axis else sum1[q, :, mine]
        sum2[q] = added(kept, [land2[q, n] for n in range(3)])
        for p in range(1, 4):
            third_sum(q, p).start()
    for q in range(4):
        for p in range(1, 4):
            third_sum(q, p).wait_recv()
        kept = sum2[q, spot_of(ORDERS[q][2], 0)]
        value = added(kept, [land3[q, n] for n in range(3)])
        out_ref[q // 2, pl.ds((q % 2) * 8, 8), :] = value

    for n in range(1, 16):
        to_peer(n).wait_send()
    for n in range(16):
        to_above(n, own).wait_send()
        to_below(n, own).wait_send()
    for y in range(2):
        to_borrower(y).wait_send()
    for y in range(4):
        to_pair(y).wait_send()
    for q in range(4):
        for p in range(1, 4):
            first_wait(q, p).wait_send()
            second_sum(q, p).wait_send()
            third_sum(q, p).wait_send()


def per_device(test_modes, modes):
    def lines(value):
        count = value.shape[0]
        value = value.reshape(count, 3, 8, 2, 2, 128).transpose(0, 1, 2, 4, 3, 5)
        return value.reshape(count * 96, 128)

    dma = pltpu.SemaphoreType.DMA
    return pl.pallas_call(
        kernel,
        out_shape=jax.ShapeDtypeStruct((2, 16, 128), F32),
        in_specs=[pl.BlockSpec(memory_space=pltpu.HBM)] * 2,
        out_specs=pl.BlockSpec(memory_space=pltpu.VMEM),
        scratch_shapes=[
            pltpu.VMEM((1536, 128), F32),
            pltpu.VMEM((3072, 128), F32),
            pltpu.VMEM((16, 8, 16, 128), F32),
            pltpu.VMEM((2, 8, 8, 16, 128), F32),
            pltpu.VMEM((2, 8, 6, 16, 128), F32),
            pltpu.VMEM((2, 8, 6, 16, 128), F32),
            pltpu.VMEM((2, 2, 3, 32, 128), F32),
            pltpu.VMEM((2, 3, 32, 128), F32),
            pltpu.VMEM((3, 2, 3, 2, 128, 128), F32),
            pltpu.VMEM((1536, 256), BF16),
            pltpu.VMEM((4, 2, 4, 4, 4, 8, 128), F32),
            pltpu.VMEM((4, 4, 4, 4, 8, 128), F32),
            pltpu.VMEM((4, 3, 4, 4, 8, 128), F32),
            pltpu.VMEM((4, 4, 4, 8, 128), F32),
            pltpu.VMEM((4, 3, 4, 8, 128), F32),
            pltpu.VMEM((4, 4, 8, 128), F32),
            pltpu.VMEM((4, 3, 8, 128), F32),
            dma((2,)),
            dma((16,)),
            dma((16,)),
            dma((16,)),
            dma((16,)),
            dma((16,)),
            dma((16,)),
            dma((2,)),
            dma((2,)),
            dma((4,)),
            dma((4,)),
            dma((3, 4, 3)),
            dma((3, 4, 3)),
        ],
        compiler_params=pltpu.CompilerParams(
            collective_id=0, has_side_effects=True, vmem_limit_bytes=62 * 1024 * 1024),
    )(lines(test_modes), lines(modes))


def solution(mesh):
    in_specs = (P(None, None, None, "space", None), P("mode", None, None, "space", None))
    out_specs = P("space", "mode", None)
    return jax.shard_map(
        per_device, mesh=mesh, in_specs=in_specs, out_specs=out_specs, check_vma=False
    )
```

```python
import jax
import jax.numpy as jnp
from jax import lax
from jax.experimental import pallas as pl
from jax.experimental.pallas import tpu as pltpu
from jax.sharding import PartitionSpec as P

F32 = jnp.float32
BF16 = jnp.bfloat16
MESH = pl.DeviceIdType.MESH
SCALE = 1.0 / 12.0 / 256.0
X, Y, Z = 0, 1, 2
PEERS = (10, 6, 14, 9, 11, 5, 15, 7, 13, 8, 2, 4, 1, 12, 3)
ORDERS = ((X, Y, Z), (Y, Z, X), (Z, X, Y), (Y, X, Z))


def rem(value, size):
    return lax.rem(value, jnp.int32(size)) if isinstance(value, jax.Array) else value % size


def div(value, size):
    return lax.div(value, jnp.int32(size)) if isinstance(value, jax.Array) else value // size


def kernel(test_hbm, mode_hbm, out_ref, x_modes, x_tests, sent, got, up, down, tests, lent,
           grads, rhs, part, paired, land1, sum1, land2, sum2, land3, load_sem, a2a_send, a2a_recv,
           up_send, down_send, up_recv, down_recv, test_send, test_recv, pair_send, pair_recv, red_send, red_recv):
    s = lax.axis_index("space")
    m = lax.axis_index("mode")
    core = rem(s, 2)
    cy = rem(div(s, 2), 4)
    zlo = div(s, 8)
    cx = div(m, 2)
    zhi = rem(m, 2)
    cz = zhi * 2 + zlo
    place = (cx, cy, cz)

    def device(x, y, z, c):
        return (rem(z, 2) * 8 + y * 2 + c, x * 2 + div(z, 2))

    def shifted(axis, step):
        there = list(place)
        there[axis] = rem(there[axis] + step, 4)
        return device(*there, core)

    load_modes = pltpu.make_async_copy(mode_hbm, x_modes, load_sem.at[0])
    load_tests = pltpu.make_async_copy(test_hbm, x_tests, load_sem.at[1])
    load_modes.start()
    load_tests.start()

    barrier = pltpu.get_barrier_semaphore()
    spot = cy * 2 + core

    def ring(step):
        there = rem(spot + step + 8, 8)
        return device(cx, div(there, 2), cz, rem(there, 2))

    def in_plane(n):
        return device(rem(cx + div(n, 4), 4), cy, rem(cz + rem(n, 4), 4), core)

    friends = [in_plane(n) for n in range(1, 16)]
    friends += [ring(1), ring(-1)]
    friends += [shifted(Y, p) for p in range(1, 4)]
    for friend in friends:
        pl.semaphore_signal(barrier, inc=1, device_id=friend, device_id_type=MESH)

    lane = lax.broadcasted_iota(jnp.int32, (8, 128), 1)
    within = lane % 16
    group = lane // 16

    load_modes.wait()

    def arrange(n, carry):
        y, a = div(n, 3), rem(n, 3)
        for xt in range(2):
            for kh in range(2):
                rows = [
                    x_modes[pl.ds(a * 32 + y + kh * 768 + z * 4 + xt * 2, 8, stride=96), :]
                    for z in range(8)
                ]
                for step in (4, 2, 1):
                    low = (group // step) % 2 == 0
                    for z in range(8):
                        if (z // step) % 2 == 0:
                            first, second = rows[z], rows[z + step]
                            rows[z] = jnp.where(low, first, pltpu.roll(second, 16 * step, 1))
                            rows[z + step] = jnp.where(
                                low, pltpu.roll(first, 128 - 16 * step, 1), second)
                for c in range(8):
                    sent[xt * 8 + c, pl.ds(n * 16 + kh * 8, 8), :] = rows[c]
        return carry

    lax.fori_loop(0, 6, arrange, 0)

    def edges(d, carry):
        left, right = rem(d + 15, 16), rem(d + 1, 16)
        for n in range(3):
            packed = jnp.zeros((8, 128), F32)
            for slot in range(4):
                kh, tile = (4 * n + slot) // 6, (4 * n + slot) % 6
                rows = pl.ds(tile * 16 + kh * 8, 8)
                turn = 4 * slot - 14
                from_left = pltpu.roll(sent[left, rows, :], (turn - 16) % 128, 1)
                from_right = pltpu.roll(sent[right, rows, :], (turn + 16) % 128, 1)
                place_in = within - 4 * slot
                packed = jnp.where((place_in == 0) | (place_in == 1), from_left, packed)
                packed = jnp.where((place_in == 2) | (place_in == 3), from_right, packed)
            sent[d, pl.ds(96 + n * 8, 8), :] = packed
        return carry

    lax.fori_loop(0, 16, edges, 0)

    pl.semaphore_wait(barrier, len(friends))

    def source(n):
        x, z = rem(cx + 4 - div(n, 4), 4), rem(cz + 4 - rem(n, 4), 4)
        return rem(z, 2), x * 2 + div(z, 2)

    def to_peer(n):
        column = rem(cx + div(n, 4), 4) * 4 + rem(cz + rem(n, 4), 4)
        return pltpu.make_async_remote_copy(
            src_ref=sent.at[column], dst_ref=got.at[zlo, m],
            send_sem=a2a_send.at[n], recv_sem=a2a_recv.at[n],
            device_id=in_plane(n), device_id_type=MESH)

    def to_above(n, src):
        slab, k = source(n)
        slab = rem(slab + div(spot, 7), 2)
        return pltpu.make_async_remote_copy(
            src_ref=src, dst_ref=down.at[slab, k],
            send_sem=up_send.at[n], recv_sem=down_recv.at[slab * 8 + k],
            device_id=ring(1), device_id_type=MESH)

    def to_below(n, src):
        slab, k = source(n)
        slab = rem(slab + div(7 - spot, 7), 2)
        return pltpu.make_async_remote_copy(
            src_ref=src, dst_ref=up.at[slab, k],
            send_sem=down_send.at[n], recv_sem=up_recv.at[slab * 8 + k],
            device_id=ring(-1), device_id_type=MESH)

    def from_ring(slab, k):
        for buffer, sems, sends in ((down, down_recv, up_send), (up, up_recv, down_send)):
            pltpu.make_async_remote_copy(
                src_ref=got.at[slab, k, pl.ds(0, 96)], dst_ref=buffer.at[slab, k],
                send_sem=sends.at[0], recv_sem=sems.at[slab * 8 + k],
                device_id=ring(1), device_id_type=MESH).wait_recv()

    own = sent.at[cx * 4 + cz, pl.ds(0, 96)]
    for n in PEERS:
        to_peer(n).start()
    to_above(0, own).start()
    to_below(0, own).start()

    load_tests.wait()

    def arrange_tests(y):
        c_mine = rem(cx, 2) * 4 + cz
        c_lent = rem(cx, 2) * 4 + rem(cz + (1 if y == 0 else 3), 4)

        def one(a, carry):
            for ih in range(4):
                start = a * 32 + y + div(cx, 2) * 2 + ih * 768
                turned = [
                    pltpu.roll(x_tests[pl.ds(start + z * 4, 8, stride=96), :], 16 * z, 1)
                    if z else x_tests[pl.ds(start, 8, stride=96), :]
                    for z in range(8)
                ]

                def pick(c):
                    value = turned[0]
                    for z in range(1, 8):
                        value = jnp.where((group + 8 - z) % 8 == c, turned[z], value)
                    return pltpu.roll(value, (128 - 16 * c) % 128, 1)

                rows = pl.ds(ih * 8, 8)
                tests[zlo, y, a, rows, :] = pick(c_mine)
                lent[y, a, rows, :] = pick(c_lent)
            return carry

        lax.fori_loop(0, 3, one, 0)

    def to_borrower(y):
        return pltpu.make_async_remote_copy(
            src_ref=lent.at[y], dst_ref=tests.at[zlo, y],
            send_sem=test_send.at[y], recv_sem=test_recv.at[y],
            device_id=shifted(Z, 1 if y == 0 else 3), device_id_type=MESH)

    def wait_tests(y):
        pltpu.make_async_remote_copy(
            src_ref=lent.at[y], dst_ref=tests.at[1 - zlo, y],
            send_sem=test_send.at[y], recv_sem=test_recv.at[y],
            device_id=shifted(Z, 1 if y == 0 else 3), device_id_type=MESH).wait_recv()

    for y in range(2):
        arrange_tests(y)
        to_borrower(y).start()

    def split(value):
        high = value.astype(BF16)
        return high, (value - high.astype(F32)).astype(BF16)

    def first_grads(n):
        slab, k = source(n)
        for tile in range(6):
            for kh in range(2):
                y, a = tile // 3, tile % 3
                rows = pl.ds(pl.multiple_of(k * 16 + kh * 8, 8), 8)
                f = got[slab, k, tile * 16 + kh * 8 : tile * 16 + kh * 8 + 8]
                near = pltpu.roll(f, 112, 1) - pltpu.roll(f, 16, 1)
                far = pltpu.roll(f, 96, 1) - pltpu.roll(f, 32, 1)
                grads[2, y, a, slab, rows, :] = (8.0 * near - far) * SCALE
                item = kh * 6 + tile
                packed = got[slab, k, 96 + item // 4 * 8 : 104 + item // 4 * 8]

                def at_edge(step, edge):
                    moved = pltpu.roll(f, step % 128, 1)
                    halo = pltpu.roll(packed, (14 - 4 * (item % 4) + step) % 128, 1)
                    return jnp.where(edge, halo, moved)

                near = at_edge(-1, within == 15) - at_edge(1, within == 0)
                far = at_edge(-2, within >= 14) - at_edge(2, within <= 1)
                grads[0, y, a, slab, rows, :] = (8.0 * near - far) * SCALE

    def second_grads(n):
        slab, k = source(n)
        from_ring(slab, k)
        rows = pl.ds(pl.multiple_of(k * 16, 16), 16)
        for a in range(3):
            f0, f1 = got[slab, k, a * 16 : a * 16 + 16], got[slab, k, a * 16 + 48 : a * 16 + 64]
            f2, f3 = up[slab, k, a * 16 : a * 16 + 16], up[slab, k, a * 16 + 48 : a * 16 + 64]
            b2, b1 = down[slab, k, a * 16 : a * 16 + 16], down[slab, k, a * 16 + 48 : a * 16 + 64]
            grads[1, 0, a, slab, rows, :] = (8.0 * (f1 - b1) - (f2 - b2)) * SCALE
            grads[1, 1, a, slab, rows, :] = (8.0 * (f2 - f0) - (f3 - b1)) * SCALE

    def arrival(n):
        slab, k = source(n)
        to_peer(n).wait_recv()
        block = got.at[slab, k, pl.ds(0, 96)]
        to_above(n, block).start()
        to_below(n, block).start()

    def turn_modes(y):
        def turn_tile(n, carry):
            tile = pl.ds(pl.multiple_of((y * 3 + div(n, 2)) * 16, 16), 16)
            field = got[rem(n, 2), :, tile, :].reshape(128, 128).T
            high, low = split(field)
            rows = pl.ds(pl.multiple_of((div(n, 2) * 4 + y * 2 + rem(n, 2)) * 128, 128), 128)
            rhs[rows, 0:128] = high
            rhs[rows, 128:256] = low
            return carry

        lax.fori_loop(0, 6, turn_tile, 0)

    def triads(c, y, terms):
        values = []
        for n in range(4):
            zl, r = n // 2, n % 2
            i = (zl * 8 + y * 2 + c) * 2 + r
            total = None
            for b, row in terms:
                columns = []
                for slab in range(2):
                    value = None
                    for a in range(3):
                        line = tests[slab, row, a, pl.ds(i, 1), :]
                        term = line * grads[b, row, a, slab]
                        value = term if value is None else value + term
                    columns.append(value)
                right = rhs[(b * 4 + row * 2) * 128 : (b * 4 + row * 2 + 2) * 128, :]
                high, low = split(jnp.concatenate(columns, axis=1))
                piece = jnp.dot(jnp.concatenate([high, low], axis=0), right, preferred_element_type=F32)
                total = piece if total is None else total + piece
            high, low = total[:128], total[128:]
            values.append((high[:, :128] + high[:, 128:]) + (low[:, :128] + low[:, 128:]))
        return values

    def step(c, y, terms, add):
        values = triads(c, y, terms)
        for n in range(4):
            zl, r = n // 2, n % 2
            for v in range(16):
                spot = (r * 2 + v % 2, c, y, v // 4, zl * 2 + (v // 2) % 2)
                piece = values[n][v * 8 : v * 8 + 8]
                part[spot] = part[spot] + piece if add else piece

    got[zlo, m] = sent[cx * 4 + cz]
    first_grads(0)
    for n in PEERS:
        arrival(n)
        first_grads(n)
    for y in range(2):
        turn_modes(y)
        wait_tests(y)

    def phase1(p, carry):
        step(rem(p, 2), div(p, 2), ((0, 0), (2, 0), (0, 1), (2, 1)), False)
        return carry

    lax.fori_loop(0, 8, phase1, 0)

    def halos(n, carry):
        second_grads(n)
        return carry

    lax.fori_loop(0, 16, halos, 0)

    def plane(z):
        return rem(z, 2) * 2 + div(z, 2)

    def spot_of(axis, step):
        there = rem(place[axis] + step, 4)
        return plane(there) if axis == Z else there

    def to_pair(y):
        return pltpu.make_async_remote_copy(
            src_ref=part.at[:, 1 - core, y], dst_ref=paired.at[y],
            send_sem=pair_send.at[y], recv_sem=pair_recv.at[y],
            device_id=device(cx, cy, cz, 1 - core), device_id_type=MESH)

    def first_sum(q, p, y):
        axis = ORDERS[q][0]
        there = spot_of(axis, p)
        if axis == Y:
            src, dst = part.at[q, core, y], land1.at[q, p - 1]
        elif axis == X:
            src, dst = part.at[q, core, y, there], land1.at[q, p - 1, y]
        else:
            src, dst = part.at[q, core, y, :, there], land1.at[q, p - 1, y]
        return pltpu.make_async_remote_copy(
            src_ref=src, dst_ref=dst,
            send_sem=red_send.at[0, q, p - 1], recv_sem=red_recv.at[0, q, p - 1],
            device_id=shifted(axis, p), device_id_type=MESH)

    def first_wait(q, p):
        axis = ORDERS[q][0]
        return pltpu.make_async_remote_copy(
            src_ref=sum1.at[q], dst_ref=land1.at[q, p - 1],
            send_sem=red_send.at[0, q, p - 1], recv_sem=red_recv.at[0, q, p - 1],
            device_id=shifted(axis, p), device_id_type=MESH)

    def finish_group(g):
        y = rem(cy + g + 1, 4)
        to_pair(y).wait_recv()
        for q in range(4):
            part[q, core, y] = part[q, core, y] + paired[y, q]
        for q in range(4):
            if ORDERS[q][0] == Y:
                if g < 3:
                    first_sum(q, g + 1, y).start()
            else:
                for p in range(1, 4):
                    first_sum(q, p, y).start()

    for g in range(4):
        y = rem(cy + g + 1, 4)

        def phase3(h, carry):
            c = jnp.where(h == 0, 1 - core, core)
            step(c, y, ((1, 0), (1, 1)), True)

            @pl.when(h == 0)
            def _():
                to_pair(y).start()

            return carry

        lax.fori_loop(0, 2, phase3, 0)
        if g > 0:
            finish_group(g - 1)
    finish_group(3)

    def dims_after(q):
        return [axis for axis in (Y, X, Z) if axis != ORDERS[q][0]]

    def second_sum(q, p):
        axis = ORDERS[q][1]
        there = spot_of(axis, p)
        src = sum1.at[q, there] if dims_after(q)[0] == axis else sum1.at[q, :, there]
        return pltpu.make_async_remote_copy(
            src_ref=src, dst_ref=land2.at[q, p - 1],
            send_sem=red_send.at[1, q, p - 1], recv_sem=red_recv.at[1, q, p - 1],
            device_id=shifted(axis, p), device_id_type=MESH)

    def third_sum(q, p):
        axis = ORDERS[q][2]
        return pltpu.make_async_remote_copy(
            src_ref=sum2.at[q, spot_of(axis, p)], dst_ref=land3.at[q, p - 1],
            send_sem=red_send.at[2, q, p - 1], recv_sem=red_recv.at[2, q, p - 1],
            device_id=shifted(axis, p), device_id_type=MESH)

    def added(kept, landing):
        return (kept + landing[0]) + (landing[1] + landing[2])

    for q in range(4):
        for p in range(1, 4):
            first_wait(q, p).wait_recv()
        axis = ORDERS[q][0]
        mine = spot_of(axis, 0)
        if axis == Y:
            kept = part[q, core, mine]
        elif axis == X:
            kept = part[q, core, :, mine]
        else:
            kept = part[q, core, :, :, mine]
        sum1[q] = added(kept, [land1[q, n] for n in range(3)])
        for p in range(1, 4):
            second_sum(q, p).start()
    for q in range(4):
        for p in range(1, 4):
            second_sum(q, p).wait_recv()
        axis = ORDERS[q][1]
        mine = spot_of(axis, 0)
        kept = sum1[q, mine] if dims_after(q)[0] == axis else sum1[q, :, mine]
        sum2[q] = added(kept, [land2[q, n] for n in range(3)])
        for p in range(1, 4):
            third_sum(q, p).start()
    for q in range(4):
        for p in range(1, 4):
            third_sum(q, p).wait_recv()
        kept = sum2[q, spot_of(ORDERS[q][2], 0)]
        value = added(kept, [land3[q, n] for n in range(3)])
        out_ref[q // 2, pl.ds((q % 2) * 8, 8), :] = value

    for n in PEERS:
        to_peer(n).wait_send()
    for n in range(16):
        to_above(n, own).wait_send()
        to_below(n, own).wait_send()
    for y in range(2):
        to_borrower(y).wait_send()
    for y in range(4):
        to_pair(y).wait_send()
    for q in range(4):
        for p in range(1, 4):
            first_wait(q, p).wait_send()
            second_sum(q, p).wait_send()
            third_sum(q, p).wait_send()


def per_device(test_modes, modes):
    def lines(value):
        count = value.shape[0]
        value = value.reshape(count, 3, 8, 2, 2, 128).transpose(0, 1, 2, 4, 3, 5)
        return value.reshape(count * 96, 128)

    dma = pltpu.SemaphoreType.DMA
    return pl.pallas_call(
        kernel,
        out_shape=jax.ShapeDtypeStruct((2, 16, 128), F32),
        in_specs=[pl.BlockSpec(memory_space=pltpu.HBM)] * 2,
        out_specs=pl.BlockSpec(memory_space=pltpu.VMEM),
        scratch_shapes=[
            pltpu.VMEM((1536, 128), F32),
            pltpu.VMEM((3072, 128), F32),
            pltpu.VMEM((16, 120, 128), F32),
            pltpu.VMEM((2, 8, 120, 128), F32),
            pltpu.VMEM((2, 8, 96, 128), F32),
            pltpu.VMEM((2, 8, 96, 128), F32),
            pltpu.VMEM((2, 2, 3, 32, 128), F32),
            pltpu.VMEM((2, 3, 32, 128), F32),
            pltpu.VMEM((3, 2, 3, 2, 128, 128), F32),
            pltpu.VMEM((1536, 256), BF16),
            pltpu.VMEM((4, 2, 4, 4, 4, 8, 128), F32),
            pltpu.VMEM((4, 4, 4, 4, 8, 128), F32),
            pltpu.VMEM((4, 3, 4, 4, 8, 128), F32),
            pltpu.VMEM((4, 4, 4, 8, 128), F32),
            pltpu.VMEM((4, 3, 4, 8, 128), F32),
            pltpu.VMEM((4, 4, 8, 128), F32),
            pltpu.VMEM((4, 3, 8, 128), F32),
            dma((2,)),
            dma((16,)),
            dma((16,)),
            dma((16,)),
            dma((16,)),
            dma((16,)),
            dma((16,)),
            dma((2,)),
            dma((2,)),
            dma((4,)),
            dma((4,)),
            dma((3, 4, 3)),
            dma((3, 4, 3)),
        ],
        compiler_params=pltpu.CompilerParams(
            collective_id=0, has_side_effects=True, vmem_limit_bytes=62 * 1024 * 1024),
    )(lines(test_modes), lines(modes))


def solution(mesh):
    in_specs = (P(None, None, None, "space", None), P("mode", None, None, "space", None))
    out_specs = P("space", "mode", None)
    return jax.shard_map(
        per_device, mesh=mesh, in_specs=in_specs, out_specs=out_specs, check_vma=False
    )
```

```python
import jax
import jax.numpy as jnp
from jax import lax
from jax.experimental import pallas as pl
from jax.experimental.pallas import tpu as pltpu
from jax.sharding import PartitionSpec as P

F32 = jnp.float32
BF16 = jnp.bfloat16
MESH = pl.DeviceIdType.MESH
SCALE = 1.0 / 12.0 / 256.0
X, Y, Z = 0, 1, 2
ARRIVAL = (0, 2, 1, 3)
STEPS = (2, 1, 3)
PEERS = (10, 6, 14, 9, 11, 5, 15, 7, 13, 8, 2, 4, 1, 12, 3)
ORDERS = ((X, Y, Z), (Y, Z, X), (Z, X, Y), (Z, Y, X))


def rem(value, size):
    return lax.rem(value, jnp.int32(size)) if isinstance(value, jax.Array) else value % size


def div(value, size):
    return lax.div(value, jnp.int32(size)) if isinstance(value, jax.Array) else value // size


def kernel(test_hbm, mode_hbm, out_ref, x_modes, x_tests, sent, got, up, down, tests, lent,
           grads, rhs, part, paired, land1, sum1, land2, sum2, land3, load_sem, a2a_send, a2a_recv,
           up_send, down_send, up_recv, down_recv, test_send, test_recv, pair_send, pair_recv, red_send, red_recv):
    s = lax.axis_index("space")
    m = lax.axis_index("mode")
    core = rem(s, 2)
    cy = rem(div(s, 2), 4)
    zlo = div(s, 8)
    cx = div(m, 2)
    zhi = rem(m, 2)
    cz = zhi * 2 + zlo
    place = (cx, cy, cz)

    def device(x, y, z, c):
        return (rem(z, 2) * 8 + y * 2 + c, x * 2 + div(z, 2))

    def shifted(axis, step):
        there = list(place)
        there[axis] = rem(there[axis] + step, 4)
        return device(*there, core)

    load_modes = pltpu.make_async_copy(mode_hbm, x_modes, load_sem.at[0])
    load_tests = pltpu.make_async_copy(test_hbm, x_tests, load_sem.at[1])
    load_modes.start()
    load_tests.start()

    barrier = pltpu.get_barrier_semaphore()
    spot = cy * 2 + core

    def ring(step):
        there = rem(spot + step + 8, 8)
        return device(cx, div(there, 2), cz, rem(there, 2))

    def in_plane(n):
        return device(rem(cx + div(n, 4), 4), cy, rem(cz + rem(n, 4), 4), core)

    friends = [in_plane(n) for n in range(1, 16)]
    friends += [ring(1), ring(-1)]
    friends += [shifted(Y, p) for p in range(1, 4)]
    for friend in friends:
        pl.semaphore_signal(barrier, inc=1, device_id=friend, device_id_type=MESH)

    lane = lax.broadcasted_iota(jnp.int32, (8, 128), 1)
    within = lane % 16
    group = lane // 16

    load_modes.wait()

    def arrange(n, carry):
        y, a = div(n, 3), rem(n, 3)
        for xt in range(2):
            for kh in range(2):
                rows = [
                    x_modes[pl.ds(a * 32 + y + kh * 768 + z * 4 + xt * 2, 8, stride=96), :]
                    for z in range(8)
                ]
                for step in (4, 2, 1):
                    low = (group // step) % 2 == 0
                    for z in range(8):
                        if (z // step) % 2 == 0:
                            first, second = rows[z], rows[z + step]
                            rows[z] = jnp.where(low, first, pltpu.roll(second, 16 * step, 1))
                            rows[z + step] = jnp.where(
                                low, pltpu.roll(first, 128 - 16 * step, 1), second)
                for c in range(8):
                    sent[xt * 8 + c, pl.ds(n * 16 + kh * 8, 8), :] = rows[c]
        return carry

    lax.fori_loop(0, 6, arrange, 0)

    def edges(d, carry):
        left, right = rem(d + 15, 16), rem(d + 1, 16)
        for n in range(3):
            packed = jnp.zeros((8, 128), F32)
            for slot in range(4):
                kh, tile = (4 * n + slot) // 6, (4 * n + slot) % 6
                rows = pl.ds(tile * 16 + kh * 8, 8)
                turn = 4 * slot - 14
                from_left = pltpu.roll(sent[left, rows, :], (turn - 16) % 128, 1)
                from_right = pltpu.roll(sent[right, rows, :], (turn + 16) % 128, 1)
                place_in = within - 4 * slot
                packed = jnp.where((place_in == 0) | (place_in == 1), from_left, packed)
                packed = jnp.where((place_in == 2) | (place_in == 3), from_right, packed)
            sent[d, pl.ds(96 + n * 8, 8), :] = packed
        return carry

    lax.fori_loop(0, 16, edges, 0)

    pl.semaphore_wait(barrier, len(friends))

    def source(n):
        x, z = rem(cx + 4 - div(n, 4), 4), rem(cz + 4 - rem(n, 4), 4)
        return rem(z, 2), x * 2 + div(z, 2)

    def to_peer(n):
        column = rem(cx + div(n, 4), 4) * 4 + rem(cz + rem(n, 4), 4)
        return pltpu.make_async_remote_copy(
            src_ref=sent.at[column], dst_ref=got.at[zlo, m],
            send_sem=a2a_send.at[n], recv_sem=a2a_recv.at[n],
            device_id=in_plane(n), device_id_type=MESH)

    def to_above(n, src):
        slab, k = source(n)
        slab = rem(slab + div(spot, 7), 2)
        return pltpu.make_async_remote_copy(
            src_ref=src, dst_ref=down.at[slab, k],
            send_sem=up_send.at[n], recv_sem=down_recv.at[slab * 8 + k],
            device_id=ring(1), device_id_type=MESH)

    def to_below(n, src):
        slab, k = source(n)
        slab = rem(slab + div(7 - spot, 7), 2)
        return pltpu.make_async_remote_copy(
            src_ref=src, dst_ref=up.at[slab, k],
            send_sem=down_send.at[n], recv_sem=up_recv.at[slab * 8 + k],
            device_id=ring(-1), device_id_type=MESH)

    def from_ring(slab, k):
        for buffer, sems, sends in ((down, down_recv, up_send), (up, up_recv, down_send)):
            pltpu.make_async_remote_copy(
                src_ref=got.at[slab, k, pl.ds(0, 96)], dst_ref=buffer.at[slab, k],
                send_sem=sends.at[0], recv_sem=sems.at[slab * 8 + k],
                device_id=ring(1), device_id_type=MESH).wait_recv()

    own = sent.at[cx * 4 + cz, pl.ds(0, 96)]
    for n in PEERS:
        to_peer(n).start()
    to_above(0, own).start()
    to_below(0, own).start()

    load_tests.wait()

    def arrange_tests(y):
        c_mine = rem(cx, 2) * 4 + cz
        c_lent = rem(cx, 2) * 4 + rem(cz + (1 if y == 0 else 3), 4)

        def one(a, carry):
            for ih in range(4):
                start = a * 32 + y + div(cx, 2) * 2 + ih * 768
                turned = [
                    pltpu.roll(x_tests[pl.ds(start + z * 4, 8, stride=96), :], 16 * z, 1)
                    if z else x_tests[pl.ds(start, 8, stride=96), :]
                    for z in range(8)
                ]

                def pick(c):
                    value = turned[0]
                    for z in range(1, 8):
                        value = jnp.where((group + 8 - z) % 8 == c, turned[z], value)
                    return pltpu.roll(value, (128 - 16 * c) % 128, 1)

                rows = pl.ds(ih * 8, 8)
                tests[zlo, y, a, rows, :] = pick(c_mine)
                lent[y, a, rows, :] = pick(c_lent)
            return carry

        lax.fori_loop(0, 3, one, 0)

    def to_borrower(y):
        return pltpu.make_async_remote_copy(
            src_ref=lent.at[y], dst_ref=tests.at[zlo, y],
            send_sem=test_send.at[y], recv_sem=test_recv.at[y],
            device_id=shifted(Z, 1 if y == 0 else 3), device_id_type=MESH)

    def wait_tests(y):
        pltpu.make_async_remote_copy(
            src_ref=lent.at[y], dst_ref=tests.at[1 - zlo, y],
            send_sem=test_send.at[y], recv_sem=test_recv.at[y],
            device_id=shifted(Z, 1 if y == 0 else 3), device_id_type=MESH).wait_recv()

    for y in range(2):
        arrange_tests(y)
        to_borrower(y).start()

    def split(value):
        high = value.astype(BF16)
        return high, (value - high.astype(F32)).astype(BF16)

    def first_grads(n):
        slab, k = source(n)
        for tile in range(6):
            for kh in range(2):
                y, a = tile // 3, tile % 3
                rows = pl.ds(pl.multiple_of(k * 16 + kh * 8, 8), 8)
                f = got[slab, k, tile * 16 + kh * 8 : tile * 16 + kh * 8 + 8]
                near = pltpu.roll(f, 112, 1) - pltpu.roll(f, 16, 1)
                far = pltpu.roll(f, 96, 1) - pltpu.roll(f, 32, 1)
                grads[2, y, a, slab, rows, :] = (8.0 * near - far) * SCALE
                item = kh * 6 + tile
                packed = got[slab, k, 96 + item // 4 * 8 : 104 + item // 4 * 8]

                edge = pltpu.roll(packed, (14 - 4 * (item % 4)) % 128, 1)

                def moved(step, at_edge):
                    return pltpu.roll(jnp.where(at_edge, edge, f), step % 128, 1)

                near = moved(-1, within == 0) - moved(1, within == 15)
                far = moved(-2, within <= 1) - moved(2, within >= 14)
                grads[0, y, a, slab, rows, :] = (8.0 * near - far) * SCALE

    def second_grads(n):
        slab, k = source(n)
        from_ring(slab, k)
        rows = pl.ds(pl.multiple_of(k * 16, 16), 16)
        for a in range(3):
            f0, f1 = got[slab, k, a * 16 : a * 16 + 16], got[slab, k, a * 16 + 48 : a * 16 + 64]
            f2, f3 = up[slab, k, a * 16 : a * 16 + 16], up[slab, k, a * 16 + 48 : a * 16 + 64]
            b2, b1 = down[slab, k, a * 16 : a * 16 + 16], down[slab, k, a * 16 + 48 : a * 16 + 64]
            grads[1, 0, a, slab, rows, :] = (8.0 * (f1 - b1) - (f2 - b2)) * SCALE
            grads[1, 1, a, slab, rows, :] = (8.0 * (f2 - f0) - (f3 - b1)) * SCALE

    def arrival(n):
        slab, k = source(n)
        to_peer(n).wait_recv()
        block = got.at[slab, k, pl.ds(0, 96)]
        to_above(n, block).start()
        to_below(n, block).start()

    def turn_modes(b):
        def turn_tile(n, carry):
            y, slab = div(n, 2), rem(n, 2)
            tile = pl.ds(pl.multiple_of((y * 3 + b) * 16, 16), 16)
            field = got[slab, :, tile, :].reshape(128, 128).T
            high, low = split(field)
            rows = pl.ds(pl.multiple_of((b * 4 + n) * 128, 128), 128)
            rhs[rows, 0:128] = high
            rhs[rows, 128:256] = low
            return carry

        lax.fori_loop(0, 4, turn_tile, 0)

    def triads(c, y, terms):
        values = []
        for n in range(4):
            zl, r = n // 2, n % 2
            i = (zl * 8 + y * 2 + c) * 2 + r
            total = None
            for b, row in terms:
                columns = []
                for slab in range(2):
                    value = None
                    for a in range(3):
                        line = tests[slab, row, a, pl.ds(i, 1), :]
                        term = line * grads[b, row, a, slab]
                        value = term if value is None else value + term
                    columns.append(value)
                right = rhs[(b * 4 + row * 2) * 128 : (b * 4 + row * 2 + 2) * 128, :]
                high, low = split(jnp.concatenate(columns, axis=1))
                piece = jnp.dot(jnp.concatenate([high, low], axis=0), right, preferred_element_type=F32)
                total = piece if total is None else total + piece
            high, low = total[:128], total[128:]
            values.append((high[:, :128] + high[:, 128:]) + (low[:, :128] + low[:, 128:]))
        return values

    def step(c, y, terms, add):
        values = triads(c, y, terms)
        for n in range(4):
            zl, r = n // 2, n % 2
            for v in range(16):
                spot = (r * 2 + v % 2, c, y, v // 4, zl * 2 + (v // 2) % 2)
                piece = values[n][v * 8 : v * 8 + 8]
                part[spot] = part[spot] + piece if add else piece

    got[zlo, m] = sent[cx * 4 + cz]
    first_grads(0)
    for n in PEERS:
        arrival(n)
        first_grads(n)
    turn_modes(0)
    turn_modes(2)
    for y in range(2):
        wait_tests(y)

    def phase1(p, carry):
        step(rem(p, 2), div(p, 2), ((0, 0), (2, 0), (0, 1), (2, 1)), False)
        return carry

    lax.fori_loop(0, 8, phase1, 0)
    turn_modes(1)

    def halos(n, carry):
        second_grads(n)
        return carry

    lax.fori_loop(0, 16, halos, 0)

    def plane(z):
        return rem(z, 2) * 2 + div(z, 2)

    def spot_of(axis, step):
        there = rem(place[axis] + step, 4)
        return plane(there) if axis == Z else there

    def to_pair(y):
        return pltpu.make_async_remote_copy(
            src_ref=part.at[:, 1 - core, y], dst_ref=paired.at[y],
            send_sem=pair_send.at[y], recv_sem=pair_recv.at[y],
            device_id=device(cx, cy, cz, 1 - core), device_id_type=MESH)

    def first_sum(q, p, y):
        axis = ORDERS[q][0]
        there = spot_of(axis, p)
        if axis == Y:
            src, dst = part.at[q, core, y], land1.at[q, p - 1]
        elif axis == X:
            src, dst = part.at[q, core, y, there], land1.at[q, p - 1, y]
        else:
            src, dst = part.at[q, core, y, :, there], land1.at[q, p - 1, y]
        return pltpu.make_async_remote_copy(
            src_ref=src, dst_ref=dst,
            send_sem=red_send.at[0, q, p - 1], recv_sem=red_recv.at[0, q, p - 1],
            device_id=shifted(axis, p), device_id_type=MESH)

    def first_wait(q, p):
        axis = ORDERS[q][0]
        return pltpu.make_async_remote_copy(
            src_ref=sum1.at[q], dst_ref=land1.at[q, p - 1],
            send_sem=red_send.at[0, q, p - 1], recv_sem=red_recv.at[0, q, p - 1],
            device_id=shifted(axis, p), device_id_type=MESH)

    def finish_group(g):
        y = rem(cy + g + 1, 4)
        to_pair(y).wait_recv()
        for q in range(4):
            part[q, core, y] = part[q, core, y] + paired[y, q]
        for q in range(4):
            if ORDERS[q][0] == Y:
                if g < 3:
                    first_sum(q, g + 1, y).start()
            else:
                for p in STEPS:
                    first_sum(q, p, y).start()

    for g, mine in ((0, False), (1, False), (0, True), (2, False), (1, True), (3, False),
                    (2, True), (3, True)):
        y = rem(cy + g + 1, 4)
        step(core if mine else 1 - core, y, ((1, 0), (1, 1)), True)
        if mine:
            finish_group(g)
        else:
            to_pair(y).start()

    def dims_after(q):
        return [axis for axis in (Y, X, Z) if axis != ORDERS[q][0]]

    def second_sum(q, p):
        axis = ORDERS[q][1]
        there = spot_of(axis, p)
        src = sum1.at[q, there] if dims_after(q)[0] == axis else sum1.at[q, :, there]
        return pltpu.make_async_remote_copy(
            src_ref=src, dst_ref=land2.at[q, p - 1],
            send_sem=red_send.at[1, q, p - 1], recv_sem=red_recv.at[1, q, p - 1],
            device_id=shifted(axis, p), device_id_type=MESH)

    def third_sum(q, p):
        axis = ORDERS[q][2]
        return pltpu.make_async_remote_copy(
            src_ref=sum2.at[q, spot_of(axis, p)], dst_ref=land3.at[q, p - 1],
            send_sem=red_send.at[2, q, p - 1], recv_sem=red_recv.at[2, q, p - 1],
            device_id=shifted(axis, p), device_id_type=MESH)

    def added(kept, landing):
        return (kept + landing[0]) + (landing[1] + landing[2])

    for q in ARRIVAL:
        for p in range(1, 4):
            first_wait(q, p).wait_recv()
        axis = ORDERS[q][0]
        mine = spot_of(axis, 0)
        if axis == Y:
            kept = part[q, core, mine]
        elif axis == X:
            kept = part[q, core, :, mine]
        else:
            kept = part[q, core, :, :, mine]
        sum1[q] = added(kept, [land1[q, n] for n in range(3)])
        for p in STEPS:
            second_sum(q, p).start()
    for q in ARRIVAL:
        for p in range(1, 4):
            second_sum(q, p).wait_recv()
        axis = ORDERS[q][1]
        mine = spot_of(axis, 0)
        kept = sum1[q, mine] if dims_after(q)[0] == axis else sum1[q, :, mine]
        sum2[q] = added(kept, [land2[q, n] for n in range(3)])
        for p in STEPS:
            third_sum(q, p).start()
    for q in ARRIVAL:
        for p in range(1, 4):
            third_sum(q, p).wait_recv()
        kept = sum2[q, spot_of(ORDERS[q][2], 0)]
        value = added(kept, [land3[q, n] for n in range(3)])
        out_ref[q // 2, pl.ds((q % 2) * 8, 8), :] = value

    for n in PEERS:
        to_peer(n).wait_send()
    for n in range(16):
        to_above(n, own).wait_send()
        to_below(n, own).wait_send()
    for y in range(2):
        to_borrower(y).wait_send()
    for y in range(4):
        to_pair(y).wait_send()
    for q in range(4):
        for p in range(1, 4):
            first_wait(q, p).wait_send()
            second_sum(q, p).wait_send()
            third_sum(q, p).wait_send()


def per_device(test_modes, modes):
    def lines(value):
        count = value.shape[0]
        value = value.reshape(count, 3, 8, 2, 2, 128).transpose(0, 1, 2, 4, 3, 5)
        return value.reshape(count * 96, 128)

    dma = pltpu.SemaphoreType.DMA
    return pl.pallas_call(
        kernel,
        out_shape=jax.ShapeDtypeStruct((2, 16, 128), F32),
        in_specs=[pl.BlockSpec(memory_space=pltpu.HBM)] * 2,
        out_specs=pl.BlockSpec(memory_space=pltpu.VMEM),
        scratch_shapes=[
            pltpu.VMEM((1536, 128), F32),
            pltpu.VMEM((3072, 128), F32),
            pltpu.VMEM((16, 120, 128), F32),
            pltpu.VMEM((2, 8, 120, 128), F32),
            pltpu.VMEM((2, 8, 96, 128), F32),
            pltpu.VMEM((2, 8, 96, 128), F32),
            pltpu.VMEM((2, 2, 3, 32, 128), F32),
            pltpu.VMEM((2, 3, 32, 128), F32),
            pltpu.VMEM((3, 2, 3, 2, 128, 128), F32),
            pltpu.VMEM((1536, 256), BF16),
            pltpu.VMEM((4, 2, 4, 4, 4, 8, 128), F32),
            pltpu.VMEM((4, 4, 4, 4, 8, 128), F32),
            pltpu.VMEM((4, 3, 4, 4, 8, 128), F32),
            pltpu.VMEM((4, 4, 4, 8, 128), F32),
            pltpu.VMEM((4, 3, 4, 8, 128), F32),
            pltpu.VMEM((4, 4, 8, 128), F32),
            pltpu.VMEM((4, 3, 8, 128), F32),
            dma((2,)),
            dma((16,)),
            dma((16,)),
            dma((16,)),
            dma((16,)),
            dma((16,)),
            dma((16,)),
            dma((2,)),
            dma((2,)),
            dma((4,)),
            dma((4,)),
            dma((3, 4, 3)),
            dma((3, 4, 3)),
        ],
        compiler_params=pltpu.CompilerParams(
            collective_id=0, has_side_effects=True, vmem_limit_bytes=62 * 1024 * 1024),
    )(lines(test_modes), lines(modes))


def solution(mesh):
    in_specs = (P(None, None, None, "space", None), P("mode", None, None, "space", None))
    out_specs = P("space", "mode", None)
    return jax.shard_map(
        per_device, mesh=mesh, in_specs=in_specs, out_specs=out_specs, check_vma=False
    )
```

```python
import jax
import jax.numpy as jnp
from jax import lax
from jax.experimental import pallas as pl
from jax.experimental.pallas import tpu as pltpu
from jax.sharding import PartitionSpec as P

F32 = jnp.float32
BF16 = jnp.bfloat16
MESH = pl.DeviceIdType.MESH
SCALE = 1.0 / 12.0 / 256.0
X, Y, Z = 0, 1, 2
ARRIVAL = (0, 2, 1, 3)
STEPS = (2, 1, 3)
PEERS = (10, 6, 14, 9, 11, 5, 15, 7, 13, 8, 2, 4, 1, 12, 3)
ORDERS = ((X, Y, Z), (Y, Z, X), (Z, X, Y), (Z, Y, X))


def rem(value, size):
    return lax.rem(value, jnp.int32(size)) if isinstance(value, jax.Array) else value % size


def div(value, size):
    return lax.div(value, jnp.int32(size)) if isinstance(value, jax.Array) else value // size


def kernel(test_hbm, mode_hbm, out_ref, x_modes, x_tests, sent, got, up, down, tests, lent,
           grads, rhs, part, paired, land1, sum1, land2, sum2, land3, load_sem, a2a_send, a2a_recv,
           up_send, down_send, up_recv, down_recv, test_send, test_recv, pair_send, pair_recv, red_send, red_recv):
    s = lax.axis_index("space")
    m = lax.axis_index("mode")
    core = rem(s, 2)
    cy = rem(div(s, 2), 4)
    zlo = div(s, 8)
    cx = div(m, 2)
    zhi = rem(m, 2)
    cz = zhi * 2 + zlo
    place = (cx, cy, cz)

    def device(x, y, z, c):
        return (rem(z, 2) * 8 + y * 2 + c, x * 2 + div(z, 2))

    def shifted(axis, step):
        there = list(place)
        there[axis] = rem(there[axis] + step, 4)
        return device(*there, core)

    load_modes = pltpu.make_async_copy(mode_hbm, x_modes, load_sem.at[0])
    load_tests = pltpu.make_async_copy(test_hbm, x_tests, load_sem.at[1])
    load_modes.start()
    load_tests.start()

    barrier = pltpu.get_barrier_semaphore()
    spot = cy * 2 + core

    def ring(step):
        there = rem(spot + step + 8, 8)
        return device(cx, div(there, 2), cz, rem(there, 2))

    def in_plane(n):
        return device(rem(cx + div(n, 4), 4), cy, rem(cz + rem(n, 4), 4), core)

    friends = [in_plane(n) for n in range(1, 16)]
    friends += [ring(1), ring(-1)]
    friends += [shifted(Y, p) for p in range(1, 4)]
    for friend in friends:
        pl.semaphore_signal(barrier, inc=1, device_id=friend, device_id_type=MESH)

    lane = lax.broadcasted_iota(jnp.int32, (8, 128), 1)
    within = lane % 16
    group = lane // 16

    load_modes.wait()

    def arrange(n, carry):
        y, a = div(n, 3), rem(n, 3)
        for xt in range(2):
            for kh in range(2):
                rows = [
                    x_modes[pl.ds(a * 32 + y + kh * 768 + z * 4 + xt * 2, 8, stride=96), :]
                    for z in range(8)
                ]
                for step in (4, 2, 1):
                    low = (group // step) % 2 == 0
                    for z in range(8):
                        if (z // step) % 2 == 0:
                            first, second = rows[z], rows[z + step]
                            rows[z] = jnp.where(low, first, pltpu.roll(second, 16 * step, 1))
                            rows[z + step] = jnp.where(
                                low, pltpu.roll(first, 128 - 16 * step, 1), second)
                for c in range(8):
                    sent[xt * 8 + c, pl.ds(n * 16 + kh * 8, 8), :] = rows[c]
        return carry

    lax.fori_loop(0, 6, arrange, 0)

    def edges(d, carry):
        left, right = rem(d + 15, 16), rem(d + 1, 16)
        for n in range(3):
            packed = jnp.zeros((8, 128), F32)
            for slot in range(4):
                kh, tile = (4 * n + slot) // 6, (4 * n + slot) % 6
                rows = pl.ds(tile * 16 + kh * 8, 8)
                turn = 4 * slot - 14
                from_left = pltpu.roll(sent[left, rows, :], (turn - 16) % 128, 1)
                from_right = pltpu.roll(sent[right, rows, :], (turn + 16) % 128, 1)
                place_in = within - 4 * slot
                packed = jnp.where((place_in == 0) | (place_in == 1), from_left, packed)
                packed = jnp.where((place_in == 2) | (place_in == 3), from_right, packed)
            sent[d, pl.ds(96 + n * 8, 8), :] = packed
        return carry

    lax.fori_loop(0, 16, edges, 0)

    pl.semaphore_wait(barrier, len(friends))

    def source(n):
        x, z = rem(cx + 4 - div(n, 4), 4), rem(cz + 4 - rem(n, 4), 4)
        return rem(z, 2), x * 2 + div(z, 2)

    def to_peer(n):
        column = rem(cx + div(n, 4), 4) * 4 + rem(cz + rem(n, 4), 4)
        return pltpu.make_async_remote_copy(
            src_ref=sent.at[column], dst_ref=got.at[zlo, m],
            send_sem=a2a_send.at[n], recv_sem=a2a_recv.at[n],
            device_id=in_plane(n), device_id_type=MESH)

    def to_above(n, src):
        slab, k = source(n)
        slab = rem(slab + div(spot, 7), 2)
        return pltpu.make_async_remote_copy(
            src_ref=src, dst_ref=down.at[slab, k],
            send_sem=up_send.at[n], recv_sem=down_recv.at[slab * 8 + k],
            device_id=ring(1), device_id_type=MESH)

    def to_below(n, src):
        slab, k = source(n)
        slab = rem(slab + div(7 - spot, 7), 2)
        return pltpu.make_async_remote_copy(
            src_ref=src, dst_ref=up.at[slab, k],
            send_sem=down_send.at[n], recv_sem=up_recv.at[slab * 8 + k],
            device_id=ring(-1), device_id_type=MESH)

    def from_ring(slab, k):
        for buffer, sems, sends in ((down, down_recv, up_send), (up, up_recv, down_send)):
            pltpu.make_async_remote_copy(
                src_ref=got.at[slab, k, pl.ds(0, 96)], dst_ref=buffer.at[slab, k],
                send_sem=sends.at[0], recv_sem=sems.at[slab * 8 + k],
                device_id=ring(1), device_id_type=MESH).wait_recv()

    own = sent.at[cx * 4 + cz, pl.ds(0, 96)]
    for n in PEERS:
        to_peer(n).start()
    to_above(0, own).start()
    to_below(0, own).start()

    load_tests.wait()

    def arrange_tests(y):
        c_mine = rem(cx, 2) * 4 + cz
        c_lent = rem(cx, 2) * 4 + rem(cz + (1 if y == 0 else 3), 4)

        def one(a, carry):
            for ih in range(4):
                start = a * 32 + y + div(cx, 2) * 2 + ih * 768
                turned = [
                    pltpu.roll(x_tests[pl.ds(start + z * 4, 8, stride=96), :], 16 * z, 1)
                    if z else x_tests[pl.ds(start, 8, stride=96), :]
                    for z in range(8)
                ]

                def pick(c):
                    value = turned[0]
                    for z in range(1, 8):
                        value = jnp.where((group + 8 - z) % 8 == c, turned[z], value)
                    return pltpu.roll(value, (128 - 16 * c) % 128, 1)

                rows = pl.ds(ih * 8, 8)
                tests[zlo, y, a, rows, :] = pick(c_mine)
                lent[y, a, rows, :] = pick(c_lent)
            return carry

        lax.fori_loop(0, 3, one, 0)

    def to_borrower(y):
        return pltpu.make_async_remote_copy(
            src_ref=lent.at[y], dst_ref=tests.at[zlo, y],
            send_sem=test_send.at[y], recv_sem=test_recv.at[y],
            device_id=shifted(Z, 1 if y == 0 else 3), device_id_type=MESH)

    def wait_tests(y):
        pltpu.make_async_remote_copy(
            src_ref=lent.at[y], dst_ref=tests.at[1 - zlo, y],
            send_sem=test_send.at[y], recv_sem=test_recv.at[y],
            device_id=shifted(Z, 1 if y == 0 else 3), device_id_type=MESH).wait_recv()

    for y in range(2):
        arrange_tests(y)
        to_borrower(y).start()

    def split(value):
        high = value.astype(BF16)
        return high, (value - high.astype(F32)).astype(BF16)

    def first_grads(n):
        slab, k = source(n)
        for tile in range(6):
            for kh in range(2):
                y, a = tile // 3, tile % 3
                rows = pl.ds(pl.multiple_of(k * 16 + kh * 8, 8), 8)
                f = got[slab, k, tile * 16 + kh * 8 : tile * 16 + kh * 8 + 8]
                near = pltpu.roll(f, 112, 1) - pltpu.roll(f, 16, 1)
                far = pltpu.roll(f, 96, 1) - pltpu.roll(f, 32, 1)
                grads[2, y, a, slab, rows, :] = (8.0 * near - far) * SCALE
                item = kh * 6 + tile
                packed = got[slab, k, 96 + item // 4 * 8 : 104 + item // 4 * 8]

                edge = pltpu.roll(packed, (14 - 4 * (item % 4)) % 128, 1)

                def moved(step, at_edge):
                    return pltpu.roll(jnp.where(at_edge, edge, f), step % 128, 1)

                near = moved(-1, within == 0) - moved(1, within == 15)
                far = moved(-2, within <= 1) - moved(2, within >= 14)
                grads[0, y, a, slab, rows, :] = (8.0 * near - far) * SCALE

    def second_grads(n):
        slab, k = source(n)
        from_ring(slab, k)
        rows = pl.ds(pl.multiple_of(k * 16, 16), 16)
        for a in range(3):
            f0, f1 = got[slab, k, a * 16 : a * 16 + 16], got[slab, k, a * 16 + 48 : a * 16 + 64]
            f2, f3 = up[slab, k, a * 16 : a * 16 + 16], up[slab, k, a * 16 + 48 : a * 16 + 64]
            b2, b1 = down[slab, k, a * 16 : a * 16 + 16], down[slab, k, a * 16 + 48 : a * 16 + 64]
            grads[1, 0, a, slab, rows, :] = (8.0 * (f1 - b1) - (f2 - b2)) * SCALE
            grads[1, 1, a, slab, rows, :] = (8.0 * (f2 - f0) - (f3 - b1)) * SCALE

    def arrival(n):
        slab, k = source(n)
        to_peer(n).wait_recv()
        block = got.at[slab, k, pl.ds(0, 96)]
        to_above(n, block).start()
        to_below(n, block).start()

    def turn_modes(b):
        def turn_tile(n, carry):
            y, slab = div(n, 2), rem(n, 2)
            tile = pl.ds(pl.multiple_of((y * 3 + b) * 16, 16), 16)
            field = got[slab, :, tile, :].reshape(128, 128).T
            high, low = split(field)
            rows = pl.ds(pl.multiple_of((b * 4 + n) * 128, 128), 128)
            rhs[rows, 0:128] = high
            rhs[rows, 128:256] = low
            return carry

        lax.fori_loop(0, 4, turn_tile, 0)

    def triads(c, y, terms):
        values = []
        for n in range(4):
            zl, r = n // 2, n % 2
            i = (zl * 8 + y * 2 + c) * 2 + r
            total = None
            for b, row in terms:
                columns = []
                for slab in range(2):
                    value = None
                    for a in range(3):
                        line = tests[slab, row, a, pl.ds(i, 1), :]
                        term = line * grads[b, row, a, slab]
                        value = term if value is None else value + term
                    columns.append(value)
                right = rhs[(b * 4 + row * 2) * 128 : (b * 4 + row * 2 + 2) * 128, :]
                high, low = split(jnp.concatenate(columns, axis=1))
                piece = jnp.dot(jnp.concatenate([high, low], axis=0), right, preferred_element_type=F32)
                total = piece if total is None else total + piece
            high, low = total[:128], total[128:]
            values.append((high[:, :128] + high[:, 128:]) + (low[:, :128] + low[:, 128:]))
        return values

    def step(c, y, terms, add):
        values = triads(c, y, terms)
        for n in range(4):
            zl, r = n // 2, n % 2
            for v in range(16):
                spot = (r * 2 + v % 2, c, y, v // 4, zl * 2 + (v // 2) % 2)
                piece = values[n][v * 8 : v * 8 + 8]
                part[spot] = part[spot] + piece if add else piece

    got[zlo, m] = sent[cx * 4 + cz]
    first_grads(0)
    for n in PEERS:
        arrival(n)
        first_grads(n)
    turn_modes(0)
    turn_modes(2)
    for y in range(2):
        wait_tests(y)

    def phase1(y, carry):
        for c in range(2):
            step(c, y, ((0, 0), (2, 0), (0, 1), (2, 1)), False)
        return carry

    lax.fori_loop(0, 4, phase1, 0)
    turn_modes(1)

    for n in (0,) + PEERS:
        second_grads(n)

    def plane(z):
        return rem(z, 2) * 2 + div(z, 2)

    def spot_of(axis, step):
        there = rem(place[axis] + step, 4)
        return plane(there) if axis == Z else there

    def to_pair(y):
        return pltpu.make_async_remote_copy(
            src_ref=part.at[:, 1 - core, y], dst_ref=paired.at[y],
            send_sem=pair_send.at[y], recv_sem=pair_recv.at[y],
            device_id=device(cx, cy, cz, 1 - core), device_id_type=MESH)

    def first_sum(q, p, y):
        axis = ORDERS[q][0]
        there = spot_of(axis, p)
        if axis == Y:
            src, dst = part.at[q, core, y], land1.at[q, p - 1]
        elif axis == X:
            src, dst = part.at[q, core, y, there], land1.at[q, p - 1, y]
        else:
            src, dst = part.at[q, core, y, :, there], land1.at[q, p - 1, y]
        return pltpu.make_async_remote_copy(
            src_ref=src, dst_ref=dst,
            send_sem=red_send.at[0, q, p - 1], recv_sem=red_recv.at[0, q, p - 1],
            device_id=shifted(axis, p), device_id_type=MESH)

    def first_wait(q, p):
        axis = ORDERS[q][0]
        return pltpu.make_async_remote_copy(
            src_ref=sum1.at[q], dst_ref=land1.at[q, p - 1],
            send_sem=red_send.at[0, q, p - 1], recv_sem=red_recv.at[0, q, p - 1],
            device_id=shifted(axis, p), device_id_type=MESH)

    def finish_group(g):
        y = rem(cy + g + 1, 4)
        to_pair(y).wait_recv()
        for q in range(4):
            part[q, core, y] = part[q, core, y] + paired[y, q]
        for q in range(4):
            if ORDERS[q][0] == Y:
                if g < 3:
                    first_sum(q, g + 1, y).start()
            else:
                for p in STEPS:
                    first_sum(q, p, y).start()

    for g, mine in ((0, False), (1, False), (0, True), (2, False), (1, True), (3, False),
                    (2, True), (3, True)):
        y = rem(cy + g + 1, 4)
        step(core if mine else 1 - core, y, ((1, 0), (1, 1)), True)
        if mine:
            finish_group(g)
        else:
            to_pair(y).start()

    def dims_after(q):
        return [axis for axis in (Y, X, Z) if axis != ORDERS[q][0]]

    def second_sum(q, p):
        axis = ORDERS[q][1]
        there = spot_of(axis, p)
        src = sum1.at[q, there] if dims_after(q)[0] == axis else sum1.at[q, :, there]
        return pltpu.make_async_remote_copy(
            src_ref=src, dst_ref=land2.at[q, p - 1],
            send_sem=red_send.at[1, q, p - 1], recv_sem=red_recv.at[1, q, p - 1],
            device_id=shifted(axis, p), device_id_type=MESH)

    def third_sum(q, p):
        axis = ORDERS[q][2]
        return pltpu.make_async_remote_copy(
            src_ref=sum2.at[q, spot_of(axis, p)], dst_ref=land3.at[q, p - 1],
            send_sem=red_send.at[2, q, p - 1], recv_sem=red_recv.at[2, q, p - 1],
            device_id=shifted(axis, p), device_id_type=MESH)

    def added(kept, landing):
        return (kept + landing[0]) + (landing[1] + landing[2])

    for q in ARRIVAL:
        for p in range(1, 4):
            first_wait(q, p).wait_recv()
        axis = ORDERS[q][0]
        mine = spot_of(axis, 0)
        if axis == Y:
            kept = part[q, core, mine]
        elif axis == X:
            kept = part[q, core, :, mine]
        else:
            kept = part[q, core, :, :, mine]
        sum1[q] = added(kept, [land1[q, n] for n in range(3)])
        for p in STEPS:
            second_sum(q, p).start()
    for q in ARRIVAL:
        for p in range(1, 4):
            second_sum(q, p).wait_recv()
        axis = ORDERS[q][1]
        mine = spot_of(axis, 0)
        kept = sum1[q, mine] if dims_after(q)[0] == axis else sum1[q, :, mine]
        sum2[q] = added(kept, [land2[q, n] for n in range(3)])
        for p in STEPS:
            third_sum(q, p).start()
    for q in ARRIVAL:
        for p in range(1, 4):
            third_sum(q, p).wait_recv()
        kept = sum2[q, spot_of(ORDERS[q][2], 0)]
        value = added(kept, [land3[q, n] for n in range(3)])
        out_ref[q // 2, pl.ds((q % 2) * 8, 8), :] = value

    for n in PEERS:
        to_peer(n).wait_send()
    for n in range(16):
        to_above(n, own).wait_send()
        to_below(n, own).wait_send()
    for y in range(2):
        to_borrower(y).wait_send()
    for y in range(4):
        to_pair(y).wait_send()
    for q in range(4):
        for p in range(1, 4):
            first_wait(q, p).wait_send()
            second_sum(q, p).wait_send()
            third_sum(q, p).wait_send()


def per_device(test_modes, modes):
    def lines(value):
        count = value.shape[0]
        value = value.reshape(count, 3, 8, 2, 2, 128).transpose(0, 1, 2, 4, 3, 5)
        return value.reshape(count * 96, 128)

    dma = pltpu.SemaphoreType.DMA
    return pl.pallas_call(
        kernel,
        out_shape=jax.ShapeDtypeStruct((2, 16, 128), F32),
        in_specs=[pl.BlockSpec(memory_space=pltpu.HBM)] * 2,
        out_specs=pl.BlockSpec(memory_space=pltpu.VMEM),
        scratch_shapes=[
            pltpu.VMEM((1536, 128), F32),
            pltpu.VMEM((3072, 128), F32),
            pltpu.VMEM((16, 120, 128), F32),
            pltpu.VMEM((2, 8, 120, 128), F32),
            pltpu.VMEM((2, 8, 96, 128), F32),
            pltpu.VMEM((2, 8, 96, 128), F32),
            pltpu.VMEM((2, 2, 3, 32, 128), F32),
            pltpu.VMEM((2, 3, 32, 128), F32),
            pltpu.VMEM((3, 2, 3, 2, 128, 128), F32),
            pltpu.VMEM((1536, 256), BF16),
            pltpu.VMEM((4, 2, 4, 4, 4, 8, 128), F32),
            pltpu.VMEM((4, 4, 4, 4, 8, 128), F32),
            pltpu.VMEM((4, 3, 4, 4, 8, 128), F32),
            pltpu.VMEM((4, 4, 4, 8, 128), F32),
            pltpu.VMEM((4, 3, 4, 8, 128), F32),
            pltpu.VMEM((4, 4, 8, 128), F32),
            pltpu.VMEM((4, 3, 8, 128), F32),
            dma((2,)),
            dma((16,)),
            dma((16,)),
            dma((16,)),
            dma((16,)),
            dma((16,)),
            dma((16,)),
            dma((2,)),
            dma((2,)),
            dma((4,)),
            dma((4,)),
            dma((3, 4, 3)),
            dma((3, 4, 3)),
        ],
        compiler_params=pltpu.CompilerParams(
            collective_id=0, has_side_effects=True, vmem_limit_bytes=62 * 1024 * 1024),
    )(lines(test_modes), lines(modes))


def solution(mesh):
    in_specs = (P(None, None, None, "space", None), P("mode", None, None, "space", None))
    out_specs = P("space", "mode", None)
    return jax.shard_map(
        per_device, mesh=mesh, in_specs=in_specs, out_specs=out_specs, check_vma=False
    )
```

```python
import jax
import jax.numpy as jnp
from jax import lax
from jax.experimental import pallas as pl
from jax.experimental.pallas import tpu as pltpu
from jax.sharding import PartitionSpec as P

F32 = jnp.float32
BF16 = jnp.bfloat16
MESH = pl.DeviceIdType.MESH
SCALE = 1.0 / 12.0 / 256.0
X, Y, Z = 0, 1, 2
ARRIVAL = (0, 2, 1, 3)
STEPS = (2, 1, 3)
PEERS = (10, 6, 14, 9, 11, 5, 15, 7, 13, 8, 2, 4, 1, 12, 3)
ORDERS = ((X, Y, Z), (Y, Z, X), (Z, X, Y), (Z, Y, X))


def rem(value, size):
    return lax.rem(value, jnp.int32(size)) if isinstance(value, jax.Array) else value % size


def div(value, size):
    return lax.div(value, jnp.int32(size)) if isinstance(value, jax.Array) else value // size


def kernel(test_hbm, mode_hbm, out_ref, x_modes, x_tests, sent, got, up, down, tests, lent,
           grads, rhs, part, paired, land1, sum1, land2, sum2, land3, load_sem, a2a_send, a2a_recv,
           up_send, down_send, up_recv, down_recv, test_send, test_recv, pair_send, pair_recv, red_send, red_recv):
    s = lax.axis_index("space")
    m = lax.axis_index("mode")
    core = rem(s, 2)
    cy = rem(div(s, 2), 4)
    zlo = div(s, 8)
    cx = div(m, 2)
    zhi = rem(m, 2)
    cz = zhi * 2 + zlo
    place = (cx, cy, cz)

    def device(x, y, z, c):
        return (rem(z, 2) * 8 + y * 2 + c, x * 2 + div(z, 2))

    def shifted(axis, step):
        there = list(place)
        there[axis] = rem(there[axis] + step, 4)
        return device(*there, core)

    load_modes = pltpu.make_async_copy(mode_hbm, x_modes, load_sem.at[0])
    load_tests = pltpu.make_async_copy(test_hbm, x_tests, load_sem.at[1])
    load_modes.start()
    load_tests.start()

    barrier = pltpu.get_barrier_semaphore()
    spot = cy * 2 + core

    def ring(step):
        there = rem(spot + step + 8, 8)
        return device(cx, div(there, 2), cz, rem(there, 2))

    def in_plane(n):
        return device(rem(cx + div(n, 4), 4), cy, rem(cz + rem(n, 4), 4), core)

    friends = [in_plane(n) for n in range(1, 16)]
    friends += [ring(1), ring(-1)]
    friends += [shifted(Y, p) for p in range(1, 4)]
    for friend in friends:
        pl.semaphore_signal(barrier, inc=1, device_id=friend, device_id_type=MESH)

    lane = lax.broadcasted_iota(jnp.int32, (8, 128), 1)
    within = lane % 16
    group = lane // 16

    load_modes.wait()

    def arrange(n, carry):
        y, a = div(n, 3), rem(n, 3)
        for xt in range(2):
            for kh in range(2):
                rows = [
                    x_modes[pl.ds(a * 32 + y + kh * 768 + z * 4 + xt * 2, 8, stride=96), :]
                    for z in range(8)
                ]
                for step in (4, 2, 1):
                    low = (group // step) % 2 == 0
                    for z in range(8):
                        if (z // step) % 2 == 0:
                            first, second = rows[z], rows[z + step]
                            rows[z] = jnp.where(low, first, pltpu.roll(second, 16 * step, 1))
                            rows[z + step] = jnp.where(
                                low, pltpu.roll(first, 128 - 16 * step, 1), second)
                for c in range(8):
                    sent[xt * 8 + c, pl.ds(n * 16 + kh * 8, 8), :] = rows[c]
        return carry

    lax.fori_loop(0, 6, arrange, 0)

    def edges(d, carry):
        left, right = rem(d + 15, 16), rem(d + 1, 16)
        for n in range(3):
            packed = jnp.zeros((8, 128), F32)
            for slot in range(4):
                kh, tile = (4 * n + slot) // 6, (4 * n + slot) % 6
                rows = pl.ds(tile * 16 + kh * 8, 8)
                turn = 4 * slot - 14
                from_left = pltpu.roll(sent[left, rows, :], (turn - 16) % 128, 1)
                from_right = pltpu.roll(sent[right, rows, :], (turn + 16) % 128, 1)
                place_in = within - 4 * slot
                packed = jnp.where((place_in == 0) | (place_in == 1), from_left, packed)
                packed = jnp.where((place_in == 2) | (place_in == 3), from_right, packed)
            sent[d, pl.ds(96 + n * 8, 8), :] = packed
        return carry

    lax.fori_loop(0, 16, edges, 0)

    pl.semaphore_wait(barrier, len(friends))

    def source(n):
        x, z = rem(cx + 4 - div(n, 4), 4), rem(cz + 4 - rem(n, 4), 4)
        return rem(z, 2), x * 2 + div(z, 2)

    def to_peer(n):
        column = rem(cx + div(n, 4), 4) * 4 + rem(cz + rem(n, 4), 4)
        return pltpu.make_async_remote_copy(
            src_ref=sent.at[column], dst_ref=got.at[zlo, m],
            send_sem=a2a_send.at[n], recv_sem=a2a_recv.at[n],
            device_id=in_plane(n), device_id_type=MESH)

    def to_above(n, src):
        slab, k = source(n)
        slab = rem(slab + div(spot, 7), 2)
        return pltpu.make_async_remote_copy(
            src_ref=src, dst_ref=down.at[slab, k],
            send_sem=up_send.at[n], recv_sem=down_recv.at[slab * 8 + k],
            device_id=ring(1), device_id_type=MESH)

    def to_below(n, src):
        slab, k = source(n)
        slab = rem(slab + div(7 - spot, 7), 2)
        return pltpu.make_async_remote_copy(
            src_ref=src, dst_ref=up.at[slab, k],
            send_sem=down_send.at[n], recv_sem=up_recv.at[slab * 8 + k],
            device_id=ring(-1), device_id_type=MESH)

    def from_ring(slab, k):
        for buffer, sems, sends in ((down, down_recv, up_send), (up, up_recv, down_send)):
            pltpu.make_async_remote_copy(
                src_ref=got.at[slab, k, pl.ds(0, 96)], dst_ref=buffer.at[slab, k],
                send_sem=sends.at[0], recv_sem=sems.at[slab * 8 + k],
                device_id=ring(1), device_id_type=MESH).wait_recv()

    own = sent.at[cx * 4 + cz, pl.ds(0, 96)]
    for n in PEERS:
        to_peer(n).start()
    to_above(0, own).start()
    to_below(0, own).start()

    load_tests.wait()

    def arrange_tests(y):
        c_mine = rem(cx, 2) * 4 + cz
        c_lent = rem(cx, 2) * 4 + rem(cz + (1 if y == 0 else 3), 4)

        def one(a, carry):
            for ih in range(4):
                start = a * 32 + y + div(cx, 2) * 2 + ih * 768
                turned = [
                    pltpu.roll(x_tests[pl.ds(start + z * 4, 8, stride=96), :], 16 * z, 1)
                    if z else x_tests[pl.ds(start, 8, stride=96), :]
                    for z in range(8)
                ]

                def pick(c):
                    value = turned[0]
                    for z in range(1, 8):
                        value = jnp.where((group + 8 - z) % 8 == c, turned[z], value)
                    return pltpu.roll(value, (128 - 16 * c) % 128, 1)

                rows = pl.ds(ih * 8, 8)
                tests[zlo, y, a, rows, :] = pick(c_mine)
                lent[y, a, rows, :] = pick(c_lent)
            return carry

        lax.fori_loop(0, 3, one, 0)

    def to_borrower(y):
        return pltpu.make_async_remote_copy(
            src_ref=lent.at[y], dst_ref=tests.at[zlo, y],
            send_sem=test_send.at[y], recv_sem=test_recv.at[y],
            device_id=shifted(Z, 1 if y == 0 else 3), device_id_type=MESH)

    def wait_tests(y):
        pltpu.make_async_remote_copy(
            src_ref=lent.at[y], dst_ref=tests.at[1 - zlo, y],
            send_sem=test_send.at[y], recv_sem=test_recv.at[y],
            device_id=shifted(Z, 1 if y == 0 else 3), device_id_type=MESH).wait_recv()

    for y in range(2):
        arrange_tests(y)
        to_borrower(y).start()

    def split(value):
        high = value.astype(BF16)
        return high, (value - high.astype(F32)).astype(BF16)

    def first_grads(n):
        slab, k = source(n)
        for tile in range(6):
            for kh in range(2):
                y, a = tile // 3, tile % 3
                rows = pl.ds(pl.multiple_of(k * 16 + kh * 8, 8), 8)
                f = got[slab, k, tile * 16 + kh * 8 : tile * 16 + kh * 8 + 8]
                near = pltpu.roll(f, 112, 1) - pltpu.roll(f, 16, 1)
                far = pltpu.roll(f, 96, 1) - pltpu.roll(f, 32, 1)
                grads[2, y, a, slab, rows, :] = (8.0 * near - far) * SCALE
                item = kh * 6 + tile
                packed = got[slab, k, 96 + item // 4 * 8 : 104 + item // 4 * 8]

                edge = pltpu.roll(packed, (14 - 4 * (item % 4)) % 128, 1)

                def moved(step, at_edge):
                    return pltpu.roll(jnp.where(at_edge, edge, f), step % 128, 1)

                near = moved(-1, within == 0) - moved(1, within == 15)
                far = moved(-2, within <= 1) - moved(2, within >= 14)
                grads[0, y, a, slab, rows, :] = (8.0 * near - far) * SCALE

    def second_grads(n):
        slab, k = source(n)
        from_ring(slab, k)
        rows = pl.ds(pl.multiple_of(k * 16, 16), 16)
        for a in range(3):
            f0, f1 = got[slab, k, a * 16 : a * 16 + 16], got[slab, k, a * 16 + 48 : a * 16 + 64]
            f2, f3 = up[slab, k, a * 16 : a * 16 + 16], up[slab, k, a * 16 + 48 : a * 16 + 64]
            b2, b1 = down[slab, k, a * 16 : a * 16 + 16], down[slab, k, a * 16 + 48 : a * 16 + 64]
            grads[1, 0, a, slab, rows, :] = (8.0 * (f1 - b1) - (f2 - b2)) * SCALE
            grads[1, 1, a, slab, rows, :] = (8.0 * (f2 - f0) - (f3 - b1)) * SCALE

    def arrival(n):
        slab, k = source(n)
        to_peer(n).wait_recv()
        block = got.at[slab, k, pl.ds(0, 96)]
        to_above(n, block).start()
        to_below(n, block).start()

    def turn_modes(b):
        for y in range(2):
            for slab in range(2):
                tile = (y * 3 + b) * 16
                field = got[slab, :, tile : tile + 16, :].reshape(128, 128).T
                high, low = split(field)
                row = (b * 4 + y * 2 + slab) * 128
                rhs[row : row + 128, 0:128] = high
                rhs[row : row + 128, 128:256] = low

    def triads(c, y, terms):
        values = []
        for n in range(4):
            zl, r = n // 2, n % 2
            i = (zl * 8 + y * 2 + c) * 2 + r
            total = None
            for b, row in terms:
                columns = []
                for slab in range(2):
                    value = None
                    for a in range(3):
                        line = tests[slab, row, a, pl.ds(i, 1), :]
                        term = line * grads[b, row, a, slab]
                        value = term if value is None else value + term
                    columns.append(value)
                right = rhs[(b * 4 + row * 2) * 128 : (b * 4 + row * 2 + 2) * 128, :]
                high, low = split(jnp.concatenate(columns, axis=1))
                piece = jnp.dot(jnp.concatenate([high, low], axis=0), right, preferred_element_type=F32)
                total = piece if total is None else total + piece
            high, low = total[:128], total[128:]
            values.append((high[:, :128] + high[:, 128:]) + (low[:, :128] + low[:, 128:]))
        return values

    def step(c, y, terms, add):
        values = triads(c, y, terms)
        for n in range(4):
            zl, r = n // 2, n % 2
            for v in range(16):
                spot = (r * 2 + v % 2, c, y, v // 4, zl * 2 + (v // 2) % 2)
                piece = values[n][v * 8 : v * 8 + 8]
                part[spot] = part[spot] + piece if add else piece

    got[zlo, m] = sent[cx * 4 + cz]
    first_grads(0)
    for n in PEERS:
        arrival(n)
        first_grads(n)
    turn_modes(0)
    turn_modes(2)
    for y in range(2):
        wait_tests(y)

    def phase1(y, carry):
        for c in range(2):
            step(c, y, ((0, 0), (2, 0), (0, 1), (2, 1)), False)
        return carry

    lax.fori_loop(0, 4, phase1, 0)
    turn_modes(1)

    for n in (0,) + PEERS:
        second_grads(n)

    def plane(z):
        return rem(z, 2) * 2 + div(z, 2)

    def spot_of(axis, step):
        there = rem(place[axis] + step, 4)
        return plane(there) if axis == Z else there

    def to_pair(y):
        return pltpu.make_async_remote_copy(
            src_ref=part.at[:, 1 - core, y], dst_ref=paired.at[y],
            send_sem=pair_send.at[y], recv_sem=pair_recv.at[y],
            device_id=device(cx, cy, cz, 1 - core), device_id_type=MESH)

    def first_sum(q, p, y):
        axis = ORDERS[q][0]
        there = spot_of(axis, p)
        if axis == Y:
            src, dst = part.at[q, core, y], land1.at[q, p - 1]
        elif axis == X:
            src, dst = part.at[q, core, y, there], land1.at[q, p - 1, y]
        else:
            src, dst = part.at[q, core, y, :, there], land1.at[q, p - 1, y]
        return pltpu.make_async_remote_copy(
            src_ref=src, dst_ref=dst,
            send_sem=red_send.at[0, q, p - 1], recv_sem=red_recv.at[0, q, p - 1],
            device_id=shifted(axis, p), device_id_type=MESH)

    def first_wait(q, p):
        axis = ORDERS[q][0]
        return pltpu.make_async_remote_copy(
            src_ref=sum1.at[q], dst_ref=land1.at[q, p - 1],
            send_sem=red_send.at[0, q, p - 1], recv_sem=red_recv.at[0, q, p - 1],
            device_id=shifted(axis, p), device_id_type=MESH)

    def finish_group(g):
        y = rem(cy + g + 1, 4)
        to_pair(y).wait_recv()
        for q in range(4):
            part[q, core, y] = part[q, core, y] + paired[y, q]
        for q in range(4):
            if ORDERS[q][0] == Y:
                if g < 3:
                    first_sum(q, g + 1, y).start()
            else:
                for p in STEPS:
                    first_sum(q, p, y).start()

    for g, mine in ((0, False), (1, False), (0, True), (2, False), (1, True), (3, False),
                    (2, True), (3, True)):
        y = rem(cy + g + 1, 4)
        step(core if mine else 1 - core, y, ((1, 0), (1, 1)), True)
        if mine:
            finish_group(g)
        else:
            to_pair(y).start()

    def dims_after(q):
        return [axis for axis in (Y, X, Z) if axis != ORDERS[q][0]]

    def second_sum(q, p):
        axis = ORDERS[q][1]
        there = spot_of(axis, p)
        src = sum1.at[q, there] if dims_after(q)[0] == axis else sum1.at[q, :, there]
        return pltpu.make_async_remote_copy(
            src_ref=src, dst_ref=land2.at[q, p - 1],
            send_sem=red_send.at[1, q, p - 1], recv_sem=red_recv.at[1, q, p - 1],
            device_id=shifted(axis, p), device_id_type=MESH)

    def third_sum(q, p):
        axis = ORDERS[q][2]
        return pltpu.make_async_remote_copy(
            src_ref=sum2.at[q, spot_of(axis, p)], dst_ref=land3.at[q, p - 1],
            send_sem=red_send.at[2, q, p - 1], recv_sem=red_recv.at[2, q, p - 1],
            device_id=shifted(axis, p), device_id_type=MESH)

    def added(kept, landing):
        return (kept + landing[0]) + (landing[1] + landing[2])

    for q in ARRIVAL:
        for p in range(1, 4):
            first_wait(q, p).wait_recv()
        axis = ORDERS[q][0]
        mine = spot_of(axis, 0)
        if axis == Y:
            kept = part[q, core, mine]
        elif axis == X:
            kept = part[q, core, :, mine]
        else:
            kept = part[q, core, :, :, mine]
        sum1[q] = added(kept, [land1[q, n] for n in range(3)])
        for p in STEPS:
            second_sum(q, p).start()
    for q in ARRIVAL:
        for p in range(1, 4):
            second_sum(q, p).wait_recv()
        axis = ORDERS[q][1]
        mine = spot_of(axis, 0)
        kept = sum1[q, mine] if dims_after(q)[0] == axis else sum1[q, :, mine]
        sum2[q] = added(kept, [land2[q, n] for n in range(3)])
        for p in STEPS:
            third_sum(q, p).start()
    for q in ARRIVAL:
        for p in range(1, 4):
            third_sum(q, p).wait_recv()
        kept = sum2[q, spot_of(ORDERS[q][2], 0)]
        value = added(kept, [land3[q, n] for n in range(3)])
        out_ref[q // 2, pl.ds((q % 2) * 8, 8), :] = value

    for n in PEERS:
        to_peer(n).wait_send()
    for n in range(16):
        to_above(n, own).wait_send()
        to_below(n, own).wait_send()
    for y in range(2):
        to_borrower(y).wait_send()
    for y in range(4):
        to_pair(y).wait_send()
    for q in range(4):
        for p in range(1, 4):
            first_wait(q, p).wait_send()
            second_sum(q, p).wait_send()
            third_sum(q, p).wait_send()


def per_device(test_modes, modes):
    def lines(value):
        count = value.shape[0]
        value = value.reshape(count, 3, 8, 2, 2, 128).transpose(0, 1, 2, 4, 3, 5)
        return value.reshape(count * 96, 128)

    dma = pltpu.SemaphoreType.DMA
    return pl.pallas_call(
        kernel,
        out_shape=jax.ShapeDtypeStruct((2, 16, 128), F32),
        in_specs=[pl.BlockSpec(memory_space=pltpu.HBM)] * 2,
        out_specs=pl.BlockSpec(memory_space=pltpu.VMEM),
        scratch_shapes=[
            pltpu.VMEM((1536, 128), F32),
            pltpu.VMEM((3072, 128), F32),
            pltpu.VMEM((16, 120, 128), F32),
            pltpu.VMEM((2, 8, 120, 128), F32),
            pltpu.VMEM((2, 8, 96, 128), F32),
            pltpu.VMEM((2, 8, 96, 128), F32),
            pltpu.VMEM((2, 2, 3, 32, 128), F32),
            pltpu.VMEM((2, 3, 32, 128), F32),
            pltpu.VMEM((3, 2, 3, 2, 128, 128), F32),
            pltpu.VMEM((1536, 256), BF16),
            pltpu.VMEM((4, 2, 4, 4, 4, 8, 128), F32),
            pltpu.VMEM((4, 4, 4, 4, 8, 128), F32),
            pltpu.VMEM((4, 3, 4, 4, 8, 128), F32),
            pltpu.VMEM((4, 4, 4, 8, 128), F32),
            pltpu.VMEM((4, 3, 4, 8, 128), F32),
            pltpu.VMEM((4, 4, 8, 128), F32),
            pltpu.VMEM((4, 3, 8, 128), F32),
            dma((2,)),
            dma((16,)),
            dma((16,)),
            dma((16,)),
            dma((16,)),
            dma((16,)),
            dma((16,)),
            dma((2,)),
            dma((2,)),
            dma((4,)),
            dma((4,)),
            dma((3, 4, 3)),
            dma((3, 4, 3)),
        ],
        compiler_params=pltpu.CompilerParams(
            collective_id=0, has_side_effects=True, vmem_limit_bytes=62 * 1024 * 1024),
    )(lines(test_modes), lines(modes))


def solution(mesh):
    in_specs = (P(None, None, None, "space", None), P("mode", None, None, "space", None))
    out_specs = P("space", "mode", None)
    return jax.shard_map(
        per_device, mesh=mesh, in_specs=in_specs, out_specs=out_specs, check_vma=False
    )
```
